16 devices in a mesh: nodes: 16 (over z, y, x, core).
Axes of the slice: x: 2, y: 2, z: 2, core: 2. Of those that a mesh axis runs over, the one named last changes fastest.
Arguments:
- adjacency: bfloat16 [16384, 16384], P('nodes')
- features: bfloat16 [16384, 100], P('nodes')
- w_one: float32 [100, 256], replicated
- w_two: float32 [256, 47], replicated
- labels: int32 [16384], P('nodes')
- label_mask: int32 [16384], P('nodes')
Outputs:
- output 1: float32 [1], replicated
- output 2: float32 [100, 256], replicated
- output 3: float32 [256, 47], replicated
All inputs are finite; a program needn't handle non-finite values.
Results may differ from the reference program's by a relative error of at most 0.001.
Values are sent between devices in bfloat16 or wider.
A program may use at most 1 GiB of HBM per device.

```python
import math
import jax
import jax.numpy as jnp
from jax import lax

NODES = 16384
BLOCK_ROWS = 1024
F_IN = 100
HIDDEN = 256
CLASSES = 47

ROW_CONTRACT = (((0,), (0,)), ((), ()))
COL_CONTRACT = (((1,), (1,)), ((), ()))


def setup_inputs(seed: int = 0) -> dict:
    key_list = jax.random.split(jax.random.key(seed), 8)
    num_comms = NODES // BLOCK_ROWS
    shifts = jax.random.randint(key_list[0], (2,), 1, num_comms)
    col_ids = jnp.arange(NODES)
    col_comm = col_ids // BLOCK_ROWS
    row_ids = jnp.arange(BLOCK_ROWS)

    def draw_rows(block_idx):
        hot_cols = (col_comm == (block_idx + shifts[0]) % num_comms) | (col_comm == (block_idx + shifts[1]) % num_comms)
        edge_prob = jnp.where(hot_cols, 0.5, 0.01)
        coin_flip = jax.random.uniform(jax.random.fold_in(key_list[1], block_idx), (BLOCK_ROWS, NODES))
        self_loop = col_ids[None, :] == block_idx * BLOCK_ROWS + row_ids[:, None]
        raw_edges = jnp.where((coin_flip < edge_prob[None, :]) | self_loop, 1.0, 0.0)
        return (raw_edges / jnp.sum(raw_edges, axis=1, keepdims=True)).astype(jnp.bfloat16)

    adjacency = lax.map(draw_rows, jnp.arange(num_comms)).reshape(NODES, NODES)
    centers = jax.random.normal(key_list[2], (num_comms, F_IN))
    feat_noise = jax.random.normal(key_list[3], (NODES, F_IN))
    features = (jnp.repeat(centers, BLOCK_ROWS, axis=0) + feat_noise).astype(jnp.bfloat16)
    w_one = jax.random.normal(key_list[4], (F_IN, HIDDEN)) * math.sqrt(2.0 / F_IN)
    w_two = jax.random.normal(key_list[5], (HIDDEN, CLASSES)) * (2.0 / math.sqrt(HIDDEN))
    labels = jax.random.randint(key_list[6], (NODES,), 0, CLASSES, dtype=jnp.int32)
    drawn_mask = jax.random.randint(key_list[7], (NODES,), 0, 10, dtype=jnp.int32) < 3
    label_mask = jnp.where((jnp.arange(NODES) % 10 == 0) | drawn_mask, 1, 0).astype(jnp.int32)
    return {'adjacency': adjacency, 'features': features, 'w_one': w_one.astype(jnp.float32), 'w_two': w_two.astype(jnp.float32), 'labels': labels, 'label_mask': label_mask}


def reference(adjacency, features, w_one, w_two, labels, label_mask):
    weight_one = w_one.astype(jnp.bfloat16)
    weight_two = w_two.astype(jnp.bfloat16)
    agg_one = jnp.dot(adjacency, features, preferred_element_type=jnp.float32).astype(jnp.bfloat16)
    pre_one = jnp.dot(agg_one, weight_one, preferred_element_type=jnp.float32)
    hidden = jnp.maximum(pre_one, 0.0).astype(jnp.bfloat16)
    agg_two = jnp.dot(adjacency, hidden, preferred_element_type=jnp.float32).astype(jnp.bfloat16)
    logits = jnp.dot(agg_two, weight_two, preferred_element_type=jnp.float32)
    weight = label_mask.astype(jnp.float32)
    label_count = jnp.sum(weight)
    onehot = (labels[:, None] == jnp.arange(CLASSES)[None, :]).astype(jnp.float32)
    log_prob = jax.nn.log_softmax(logits, axis=-1)
    loss_value = -jnp.sum(weight * jnp.sum(onehot * log_prob, axis=-1)) / label_count
    grad_two = (weight[:, None] * (jnp.exp(log_prob) - onehot) / label_count).astype(jnp.bfloat16)
    dw_two = lax.dot_general(agg_two, grad_two, ROW_CONTRACT, preferred_element_type=jnp.float32)
    back_two = lax.dot_general(grad_two, weight_two, COL_CONTRACT, preferred_element_type=jnp.float32).astype(jnp.bfloat16)
    d_hidden = lax.dot_general(adjacency, back_two, ROW_CONTRACT, preferred_element_type=jnp.float32)
    grad_one = jnp.where(pre_one > 0.0, d_hidden, 0.0).astype(jnp.bfloat16)
    dw_one = lax.dot_general(agg_one, grad_one, ROW_CONTRACT, preferred_element_type=jnp.float32)
    return (loss_value.reshape(1), dw_one, dw_two)
```

```python
import functools

import jax
import jax.numpy as jnp
from jax import lax
from jax.experimental import pallas as pl
from jax.experimental.pallas import tpu as pltpu
from jax.sharding import PartitionSpec as P

MESH = pl.DeviceIdType.MESH
AXIS = 'nodes'
F32, BF16 = jnp.float32, jnp.bfloat16
NDEV = 16
BLK = 1024
FIN, FPAD = 100, 128
HID = 256
NCLS, CPAD = 47, 48
RING = 4

ORDER = ((0, 1, 2), (1, 2, 0), (2, 0, 1))
GATHER_ROWS = ((0, 352), (352, 336), (688, 336))
REDUCE_ROWS = ((0, 88), (88, 88), (176, 80))

NT = (((1,), (1,)), ((), ()))


def gather_unit(axis, slot):
    first, second, third = axis, (axis + 2) % 3, (axis + 1) % 3
    if slot == 0:
        return first, 0
    if slot == 1:
        return second, 0
    if slot == 2:
        return third, 0
    if slot == 3:
        return second, 1 << ORDER[second][0]
    one, two = 1 << ORDER[third][0], 1 << ORDER[third][1]
    return third, {4: one, 5: two, 6: one | two}[slot]


def reduce_unit(part, k):
    b1, b2, b3 = ORDER[part]
    m1, m2, m3 = 1 << b1, 1 << b2, 1 << b3
    return ((b1, m1 | m2 | m3), (b1, m1 | m2), (b1, m1 | m3), (b1, m1), (b2, m2 | m3), (b2, m2), (b3, m3))[k]


def step_order(i):
    t, j = (i + 1) // 3, (i + 1) % 3
    power = (j * j + j + 2) // 2
    late = t // 5
    one = (1 - t // 3) * ((t + 1) // 2)
    two = (t // 3) * (1 - late)
    zero = 1 - (t + 4) // 5
    mask = one * power + two * (7 - power) + late * 7
    core = zero * (j - 1) + (one + two) * ((t + 1) % 2) + late * j
    return mask, core


def flip(bit, by):
    return bit + by - 2 * bit * by


def kernel(a_hbm, x_hbm, w1_ref, w2_ref, y_ref, m_ref, loss_ref, dw1_ref, dw2_ref,
           abuf, xin, xall, hall, s1acc, s2acc, s1b, s2b, z1t, w1p, w1t, w2p, w2t, ut, acc, drecv, rbuf, gt,
           cnt, d2src, d2r1, d2r2, d1src, d1r1, d1r2,
           asem, xsem, gs, gr, ds, dr, rs, rr, es, er, ms, mr, ps, pr):
    me = lax.axis_index(AXIS)
    core, px, py, pz = me % 2, (me // 2) % 2, (me // 4) % 2, me // 8

    def dev(mask, other=0):
        fx, fy, fz, fc = mask % 2, (mask // 2) % 2, mask // 4, other
        return ((flip(pz, fz) * 2 + flip(py, fy)) * 2 + flip(px, fx)) * 2 + flip(core, fc)

    def block_of(i):
        mask, other = step_order(i)
        return dev(mask, other)

    def load_a(i, slot):
        start = pl.multiple_of(block_of(i) * BLK, BLK)
        return pltpu.make_async_copy(a_hbm.at[:, pl.ds(start, BLK)], abuf.at[slot], asem.at[slot])

    def wait_a(slot):
        pltpu.make_async_copy(a_hbm.at[:, pl.ds(0, BLK)], abuf.at[slot], asem.at[slot]).wait()

    def remote(src, dst, send, recv, to):
        return pltpu.make_async_remote_copy(src_ref=src, dst_ref=dst, send_sem=send, recv_sem=recv,
                                            device_id=(to,), device_id_type=MESH)

    def peer(d):
        return dev(d // 2, d % 2)

    far_first = sorted(range(1, NDEV), key=lambda d: -bin(d // 2).count('1'))

    x_load = pltpu.make_async_copy(x_hbm, xin, xsem.at[0])
    x_load.start()
    for i in range(RING):
        load_a(i, i).start()
    barrier = pltpu.get_barrier_semaphore()
    for d in far_first:
        pl.semaphore_signal(barrier, inc=1, device_id=(peer(d),), device_id_type=MESH)
    w1p[...] = jnp.zeros_like(w1p)
    w1p[0:FIN, :] = w1_ref[...]
    w2p[...] = jnp.zeros_like(w2p)
    w2p[:, 0:NCLS] = w2_ref[...]
    s1acc[...] = jnp.zeros_like(s1acc)
    s2acc[...] = jnp.zeros_like(s2acc)
    xall[me] = jnp.zeros((BLK, FPAD), BF16)
    x_load.wait()
    xall[me, :, 0:FIN] = xin[...]
    cnt[me] = jnp.full((8, 128), jnp.sum(m_ref[...].astype(F32)), F32)
    pl.semaphore_wait(barrier, NDEV - 1)

    def gather(buf, g):
        def copy(axis, slot, at_receiver=False):
            part, mask = gather_unit(axis, slot)
            owner = dev(mask | (1 << axis) if at_receiver else mask)
            ref = buf.at[owner, pl.ds(*GATHER_ROWS[part])]
            n = g * 21 + axis * 7 + slot
            return remote(ref, ref, gs.at[n], gr.at[n], dev(1 << axis))

        def pair(mask, at_receiver=False):
            ref = buf.at[dev(mask, 1 if at_receiver else 0)]
            return remote(ref, ref, ds.at[g * 8 + mask], dr.at[g * 8 + mask], dev(0, 1))

        def begin():
            for slot in range(3):
                for axis in range(3):
                    copy(axis, slot).start()
            pair(0).start()

        def arrive(slots):
            for slot in slots:
                for axis in range(3):
                    copy(axis, slot, True).wait_recv()
                    part, mask = gather_unit(axis, slot)
                    got = (part, mask | (1 << axis))
                    for later in range(3, 7):
                        for onto in range(3):
                            if gather_unit(onto, later) == got:
                                copy(onto, later).start()

        def hooks(i):
            @pl.when(i == 1)
            def _():
                pair(0, True).wait_recv()

            @pl.when(i == 2)
            def _():
                arrive((0, 1, 2))
                for mask in (1, 2, 4):
                    pair(mask).start()

            @pl.when(i == 8)
            def _():
                arrive((3, 4, 5))
                for mask in (6, 5, 3):
                    pair(mask).start()

            @pl.when(i == 14)
            def _():
                arrive((6,))
                pair(7).start()

            for step in (5, 6, 7, 11, 12, 13, 15):
                @pl.when(i == step)
                def _():
                    pair(step_order(step)[0], True).wait_recv()

        def drain():
            for axis in range(3):
                for slot in range(7):
                    copy(axis, slot).wait_send()
            for mask in range(8):
                pair(mask).wait_send()

        return begin, hooks, drain

    def aggregate(buf, total, hooks, g):
        @pl.loop(0, NDEV)
        def _(i):
            hooks(i)
            slot = i % RING
            wait_a(slot)
            block = block_of(i)

            @pl.loop(0, 2)
            def _(half):
                rows = pl.ds(pl.multiple_of(half * 512, 512), 512)
                total[rows, :] += jnp.dot(abuf[slot, rows, :], buf[block], preferred_element_type=F32)

            if g == 0:
                load_a((i + RING) % NDEV, slot).start()
            else:
                @pl.when(i < NDEV - RING)
                def _():
                    load_a(i + RING, slot).start()

    def count_copy(d):
        ref = cnt.at[me]
        return remote(ref, ref, ms.at[d], mr.at[d], peer(d))

    begin_x, hooks_x, drain_x = gather(xall, 0)
    begin_h, hooks_h, drain_h = gather(hall, 1)

    begin_x()
    for d in far_first:
        count_copy(d).start()
    w1t[...] = w1p[...].T.astype(BF16)
    w2t[...] = w2p[...].T.astype(BF16)
    aggregate(xall, s1acc, hooks_x, 0)

    s1b[...] = s1acc[...].astype(BF16)
    pre_one = jnp.dot(s1b[...], w1p[...].astype(BF16), preferred_element_type=F32)
    hall[me] = jnp.maximum(pre_one, 0.0).astype(BF16)
    z1t[...] = lax.dot_general(w1t[...], s1b[...], NT, preferred_element_type=F32)
    begin_h()
    aggregate(hall, s2acc, hooks_h, 1)

    for d in range(1, NDEV):
        ref = cnt.at[peer(d)]
        remote(ref, ref, ms.at[d], mr.at[d], peer(d)).wait_recv()
    label_count = jnp.sum(cnt[...], axis=0)[0:1, 0:1]
    s2b[...] = s2acc[...].astype(BF16)
    logits = lax.dot_general(w2t[...], s2b[...], NT, preferred_element_type=F32)[0:CPAD]
    classes = lax.broadcasted_iota(jnp.int32, (CPAD, BLK), 0)
    logits = jnp.where(classes < NCLS, logits, -jnp.inf)
    shifted = logits - jnp.max(logits, axis=0, keepdims=True)
    log_prob = shifted - jnp.log(jnp.sum(jnp.exp(shifted), axis=0, keepdims=True))
    hit = classes == y_ref[...]
    weight = m_ref[...].astype(F32)
    picked = jnp.sum(jnp.where(hit, log_prob, 0.0), axis=0, keepdims=True)
    loss_part = -jnp.sum(weight * picked)
    grad = weight * (jnp.exp(log_prob) - jnp.where(hit, 1.0, 0.0)) / label_count
    gt[...] = grad.astype(BF16)
    ut[...] = jnp.dot(w2p[...][:, 0:CPAD].astype(BF16), gt[...], preferred_element_type=F32).astype(BF16)

    def pair_sum(mask):
        return remote(acc.at[8 + mask], drecv.at[mask], es.at[mask], er.at[mask], dev(0, 1))

    def unit_copy(part, k):
        axis, mask = reduce_unit(part, k)
        rows = pl.ds(*REDUCE_ROWS[part])
        n = part * 7 + k
        return remote(acc.at[mask, rows], rbuf.at[k, rows], rs.at[n], rr.at[n], dev(1 << axis))

    def add_rows(mask, source, start, size):
        @pl.loop(0, size // 8)
        def _(t):
            rows = pl.ds(pl.multiple_of(start + t * 8, 8), 8)
            acc[mask, rows, :] += source[rows, :]

    def take_pair(mask):
        pair_sum(mask).wait_recv()
        add_rows(mask, drecv.at[mask], 0, HID)
        for k in range(4):
            for part in range(3):
                if reduce_unit(part, k)[1] == mask:
                    unit_copy(part, k).start()

    @pl.loop(0, NDEV)
    def _(i):
        slot = (NDEV - 1 - i) % RING
        mask, other = step_order(NDEV - 1 - i)

        @pl.when(i >= RING)
        def _():
            wait_a(slot)

        @pl.loop(0, 2)
        def _(half):
            cols = pl.ds(pl.multiple_of(half * 512, 512), 512)
            acc[mask + 8 * other, :, cols] = jnp.dot(ut[...], abuf[slot, :, cols], preferred_element_type=F32)

        @pl.when(i < NDEV - RING)
        def _():
            load_a(NDEV - 1 - i - RING, slot).start()

        for step in range(NDEV):
            step_mask, step_other = step_order(NDEV - 1 - step)

            @pl.when(i == step)
            def _():
                if step_other:
                    pair_sum(step_mask).start()
                else:
                    take_pair(step_mask)

    def small_scatter(src, dst, d, base, wait):
        if wait:
            ref = dst.at[peer(d)]
            return remote(ref, ref, ps.at[base + d], pr.at[base + d], peer(d))
        return remote(src.at[peer(d)], dst.at[me], ps.at[base + d], pr.at[base + d], peer(d))

    def small_gather(dst, d, base, wait):
        ref = dst.at[peer(d)] if wait else dst.at[me]
        return remote(ref, ref, ps.at[base + d], pr.at[base + d], peer(d))

    dw2_part = jnp.dot(gt[...], s2b[...], preferred_element_type=F32)
    d2src[...] = jnp.zeros_like(d2src)
    for j in range(6):
        d2src[j] = dw2_part[j * 8:(j + 1) * 8, 0:128]
        d2src[6 + j] = dw2_part[j * 8:(j + 1) * 8, 128:256]
    d2src[12] = jnp.full((8, 128), loss_part, F32)
    d2r1[me] = d2src[me]
    for d in far_first:
        small_scatter(d2src, d2r1, d, 0, False).start()

    def take_unit(part, k, send=None):
        axis, mask = reduce_unit(part, k)
        unit_copy(part, k).wait_recv()
        add_rows(mask - (1 << axis), rbuf.at[k], *REDUCE_ROWS[part])
        if send is not None:
            unit_copy(part, send).start()

    for part in range(3):
        take_unit(part, 0, 4)
    for part in range(3):
        take_unit(part, 1, 5)
    for part in range(3):
        take_unit(part, 2)
    for d in range(1, NDEV):
        small_scatter(d2src, d2r1, d, 0, True).wait_recv()
    d2r2[me] = jnp.sum(d2r1[...], axis=0)
    for d in far_first:
        small_gather(d2r2, d, 16, False).start()
    for part in range(3):
        take_unit(part, 3)
    for part in range(3):
        take_unit(part, 4, 6)
    for part in range(3):
        take_unit(part, 5)
    for part in range(3):
        take_unit(part, 6)

    grad_one = jnp.where(z1t[...] > 0.0, acc[0], 0.0).astype(BF16)
    d1src[...] = jnp.dot(grad_one, s1b[...], preferred_element_type=F32).reshape(NDEV, 16, FPAD)
    d1r1[me] = d1src[me]
    for d in far_first:
        small_scatter(d1src, d1r1, d, 32, False).start()
    for d in range(1, NDEV):
        small_gather(d2r2, d, 16, True).wait_recv()
    left = d2r2[0:6].reshape(CPAD, 128)
    right = d2r2[6:12].reshape(CPAD, 128)
    dw2_ref[:, :] = jnp.concatenate([left, right], axis=1).T[:, 0:NCLS]
    loss_ref[...] = d2r2[12] / label_count
    for d in range(1, NDEV):
        small_scatter(d1src, d1r1, d, 32, True).wait_recv()
    d1r2[me] = jnp.sum(d1r1[...], axis=0)
    for d in far_first:
        small_gather(d1r2, d, 48, False).start()
    drain_x()
    drain_h()
    for mask in range(8):
        pair_sum(mask).wait_send()
    for part in range(3):
        for k in range(7):
            unit_copy(part, k).wait_send()
    for d in range(1, NDEV):
        count_copy(d).wait_send()
        small_scatter(d2src, d2r1, d, 0, False).wait_send()
        small_gather(d2r2, d, 16, False).wait_send()
        small_scatter(d1src, d1r1, d, 32, False).wait_send()
    for d in range(1, NDEV):
        small_gather(d1r2, d, 48, True).wait_recv()
    dw1_ref[...] = d1r2[...].reshape(HID, FPAD).T[0:FIN, :]
    for d in range(1, NDEV):
        small_gather(d1r2, d, 48, False).wait_send()


def solution(mesh):
    def local_step(adj_rows, feat_rows, w_one, w_two, label_rows, mask_rows):
        vmem = pl.BlockSpec(memory_space=pltpu.VMEM)
        hbm = pl.BlockSpec(memory_space=pl.ANY)
        dma = pltpu.SemaphoreType.DMA
        loss, dw_one, dw_two = pl.pallas_call(
            kernel,
            out_shape=(jax.ShapeDtypeStruct((8, 128), F32), jax.ShapeDtypeStruct((FIN, HID), F32),
                       jax.ShapeDtypeStruct((HID, NCLS), F32)),
            in_specs=[hbm, hbm, vmem, vmem, vmem, vmem],
            out_specs=(vmem, vmem, vmem),
            scratch_shapes=[
                pltpu.VMEM((RING, BLK, BLK), BF16),
                pltpu.VMEM((BLK, FIN), BF16),
                pltpu.VMEM((NDEV, BLK, FPAD), BF16),
                pltpu.VMEM((NDEV, BLK, HID), BF16),
                pltpu.VMEM((BLK, FPAD), F32),
                pltpu.VMEM((BLK, HID), F32),
                pltpu.VMEM((BLK, FPAD), BF16),
                pltpu.VMEM((BLK, HID), BF16),
                pltpu.VMEM((HID, BLK), F32),
                pltpu.VMEM((FPAD, HID), F32),
                pltpu.VMEM((HID, FPAD), BF16),
                pltpu.VMEM((HID, 128), F32),
                pltpu.VMEM((128, HID), BF16),
                pltpu.VMEM((HID, BLK), BF16),
                pltpu.VMEM((16, HID, BLK), F32),
                pltpu.VMEM((8, HID, BLK), F32),
                pltpu.VMEM((7, HID, BLK), F32),
                pltpu.VMEM((CPAD, BLK), BF16),
                pltpu.VMEM((NDEV, 8, 128), F32),
                pltpu.VMEM((NDEV, 8, 128), F32),
                pltpu.VMEM((NDEV, 8, 128), F32),
                pltpu.VMEM((NDEV, 8, 128), F32),
                pltpu.VMEM((NDEV, 16, FPAD), F32),
                pltpu.VMEM((NDEV, 16, FPAD), F32),
                pltpu.VMEM((NDEV, 16, FPAD), F32),
                dma((RING,)), dma((1,)), dma((42,)), dma((42,)), dma((16,)), dma((16,)), dma((21,)), dma((21,)),
                dma((8,)), dma((8,)), dma((16,)), dma((16,)), dma((64,)), dma((64,)),
            ],
            compiler_params=pltpu.CompilerParams(collective_id=0, has_side_effects=True,
                                                 vmem_limit_bytes=66 * 1000 * 1000),
        )(adj_rows, feat_rows, w_one, w_two, label_rows.reshape(1, BLK), mask_rows.reshape(1, BLK))
        return loss[0, 0:1], dw_one, dw_two

    return jax.shard_map(local_step, mesh=mesh,
                         in_specs=(P(AXIS, None), P(AXIS, None), P(None, None), P(None, None), P(AXIS), P(AXIS)),
                         out_specs=(P(None), P(None, None), P(None, None)), check_vma=False)
```

```python
import functools

import jax
import jax.numpy as jnp
from jax import lax
from jax.experimental import pallas as pl
from jax.experimental.pallas import tpu as pltpu
from jax.sharding import PartitionSpec as P

MESH = pl.DeviceIdType.MESH
AXIS = 'nodes'
F32, BF16 = jnp.float32, jnp.bfloat16
NDEV = 16
BLK = 1024
FIN, FROWS, FPAD = 100, 104, 128
HID = 256
NCLS, CPAD = 47, 48
RING = 4

ORDER = ((0, 1, 2), (1, 2, 0), (2, 0, 1))
GATHER_ROWS = ((0, 352), (352, 336), (688, 336))
GATHER_COLS = ((0, 384), (384, 384), (768, 256))
REDUCE_ROWS = ((0, 88), (88, 88), (176, 80))

NT = (((1,), (1,)), ((), ()))
TN = (((0,), (0,)), ((), ()))


def gather_unit(axis, slot):
    first, second, third = axis, (axis + 2) % 3, (axis + 1) % 3
    if slot == 0:
        return first, 0
    if slot == 1:
        return second, 0
    if slot == 2:
        return third, 0
    if slot == 3:
        return second, 1 << ORDER[second][0]
    one, two = 1 << ORDER[third][0], 1 << ORDER[third][1]
    return third, {4: one, 5: two, 6: one | two}[slot]


def reduce_unit(part, k):
    b1, b2, b3 = ORDER[part]
    m1, m2, m3 = 1 << b1, 1 << b2, 1 << b3
    return ((b1, m1 | m2 | m3), (b1, m1 | m2), (b1, m1 | m3), (b1, m1), (b2, m2 | m3), (b2, m2), (b3, m3))[k]


def step_order(i):
    t, j = (i + 1) // 3, (i + 1) % 3
    power = (j * j + j + 2) // 2
    late = t // 5
    one = (1 - t // 3) * ((t + 1) // 2)
    two = (t // 3) * (1 - late)
    zero = 1 - (t + 4) // 5
    mask = one * power + two * (7 - power) + late * 7
    core = zero * (j - 1) + (one + two) * ((t + 1) % 2) + late * j
    return mask, core


def flip(bit, by):
    return bit + by - 2 * bit * by


def kernel(a_hbm, x_hbm, w1_hbm, w2_hbm, y_hbm, m_hbm, loss_ref, dw1_ref, dw2_ref,
           abuf, xin, w1_ref, w2_ref, y_ref, m_ref, xall, hall, s1acc, s2acc, s1b, s2b, z1t, w1p, w1t, w2t, ut,
           acc, drecv, rbuf, gt,
           cnt, d2src, d2r1, d2r2, d1src, d1r1, d1r2,
           asem, xsem, gs, gr, ds, dr, rs, rr, es, er, ms, mr, ps, pr):
    me = lax.axis_index(AXIS)
    core, px, py, pz = me % 2, (me // 2) % 2, (me // 4) % 2, me // 8

    def dev(mask, other=0):
        fx, fy, fz, fc = mask % 2, (mask // 2) % 2, mask // 4, other
        return ((flip(pz, fz) * 2 + flip(py, fy)) * 2 + flip(px, fx)) * 2 + flip(core, fc)

    def block_of(i):
        mask, other = step_order(i)
        return dev(mask, other)

    def load_a(i, slot):
        start = pl.multiple_of(block_of(i) * BLK, BLK)
        return pltpu.make_async_copy(a_hbm.at[:, pl.ds(start, BLK)], abuf.at[slot], asem.at[slot])

    def wait_a(slot):
        pltpu.make_async_copy(a_hbm.at[:, pl.ds(0, BLK)], abuf.at[slot], asem.at[slot]).wait()

    def remote(src, dst, send, recv, to):
        return pltpu.make_async_remote_copy(src_ref=src, dst_ref=dst, send_sem=send, recv_sem=recv,
                                            device_id=(to,), device_id_type=MESH)

    def peer(d):
        return dev(d // 2, d % 2)

    far_first = sorted(range(1, NDEV), key=lambda d: -bin(d // 2).count('1'))

    loads = [pltpu.make_async_copy(src, dst, xsem.at[k]) for k, (src, dst) in enumerate((
        (x_hbm, xin), (m_hbm, m_ref), (w1_hbm, w1_ref), (w2_hbm, w2_ref), (y_hbm, y_ref)))]
    for load in loads:
        load.start()
    for i in range(RING):
        load_a(i, i).start()
    barrier = pltpu.get_barrier_semaphore()
    for d in far_first:
        pl.semaphore_signal(barrier, inc=1, device_id=(peer(d),), device_id_type=MESH)
    xall[me] = jnp.zeros((FROWS, BLK), BF16)
    loads[0].wait()
    xall[me, 0:FIN, :] = xin[...]
    loads[1].wait()
    cnt[me] = jnp.full((8, 128), jnp.sum(m_ref[...].astype(F32)), F32)
    pl.semaphore_wait(barrier, NDEV - 1)

    def gather(buf, g):
        def piece(owner, part):
            return buf.at[owner, :, pl.ds(*GATHER_COLS[part])] if g == 0 else buf.at[owner, pl.ds(*GATHER_ROWS[part])]

        def copy(axis, slot, at_receiver=False):
            part, mask = gather_unit(axis, slot)
            owner = dev(mask | (1 << axis) if at_receiver else mask)
            ref = piece(owner, part)
            n = g * 21 + axis * 7 + slot
            return remote(ref, ref, gs.at[n], gr.at[n], dev(1 << axis))

        def pair(mask, at_receiver=False):
            ref = buf.at[dev(mask, 1 if at_receiver else 0)]
            return remote(ref, ref, ds.at[g * 8 + mask], dr.at[g * 8 + mask], dev(0, 1))

        def begin():
            for slot in range(3):
                for axis in range(3):
                    copy(axis, slot).start()
            pair(0).start()

        def arrive(slots):
            for slot in slots:
                for axis in range(3):
                    copy(axis, slot, True).wait_recv()
                    part, mask = gather_unit(axis, slot)
                    got = (part, mask | (1 << axis))
                    for later in range(3, 7):
                        for onto in range(3):
                            if gather_unit(onto, later) == got:
                                copy(onto, later).start()

        def hooks(i):
            @pl.when(i == 1)
            def _():
                pair(0, True).wait_recv()

            @pl.when(i == 2)
            def _():
                arrive((0, 1, 2))
                for mask in (1, 2, 4):
                    pair(mask).start()

            @pl.when(i == 8)
            def _():
                arrive((3, 4, 5))
                for mask in (6, 5, 3):
                    pair(mask).start()

            @pl.when(i == 14)
            def _():
                arrive((6,))
                pair(7).start()

            for step in (5, 6, 7, 11, 12, 13, 15):
                @pl.when(i == step)
                def _():
                    pair(step_order(step)[0], True).wait_recv()

        def drain():
            for axis in range(3):
                for slot in range(7):
                    copy(axis, slot).wait_send()
            for mask in range(8):
                pair(mask).wait_send()

        return begin, hooks, drain

    def aggregate(buf, total, hooks, g):
        @pl.loop(0, NDEV)
        def _(i):
            hooks(i)
            slot = i % RING
            wait_a(slot)
            block = block_of(i)

            @pl.loop(0, 2)
            def _(half):
                rows = pl.ds(pl.multiple_of(half * 512, 512), 512)
                if g == 0:
                    total[0:FROWS, rows] += lax.dot_general(buf[block], abuf[slot, rows, :], NT,
                                                            preferred_element_type=F32)
                else:
                    total[rows, :] += jnp.dot(abuf[slot, rows, :], buf[block], preferred_element_type=F32)

            if g == 0:
                load_a((i + RING) % NDEV, slot).start()
            else:
                @pl.when(i < NDEV - RING)
                def _():
                    load_a(i + RING, slot).start()

    def count_copy(d):
        ref = cnt.at[me]
        return remote(ref, ref, ms.at[d], mr.at[d], peer(d))

    begin_x, hooks_x, drain_x = gather(xall, 0)
    begin_h, hooks_h, drain_h = gather(hall, 1)

    begin_x()
    for d in far_first:
        count_copy(d).start()
    for load in loads[2:]:
        load.wait()
    w1p[...] = jnp.zeros_like(w1p)
    w1p[0:FIN, :] = w1_ref[...]
    w1t[...] = w1p[...].T.astype(BF16)
    w2t[...] = jnp.zeros_like(w2t)
    w2t[0:NCLS, :] = w2_ref[...].astype(BF16)
    s1acc[...] = jnp.zeros_like(s1acc)
    s2acc[...] = jnp.zeros_like(s2acc)
    aggregate(xall, s1acc, hooks_x, 0)

    s1b[...] = s1acc[...].astype(BF16)
    pre_one = jnp.dot(s1acc[...].T.astype(BF16), w1p[...].astype(BF16), preferred_element_type=F32)
    hall[me] = jnp.maximum(pre_one, 0.0).astype(BF16)
    z1t[...] = jnp.dot(w1t[...], s1b[...], preferred_element_type=F32)
    begin_h()
    aggregate(hall, s2acc, hooks_h, 1)

    for d in range(1, NDEV):
        ref = cnt.at[peer(d)]
        remote(ref, ref, ms.at[d], mr.at[d], peer(d)).wait_recv()
    label_count = jnp.sum(cnt[...], axis=0)[0:1, 0:1]
    s2b[...] = s2acc[...].astype(BF16)
    logits = lax.dot_general(w2t[...], s2b[...], NT, preferred_element_type=F32)
    classes = lax.broadcasted_iota(jnp.int32, (CPAD, BLK), 0)
    logits = jnp.where(classes < NCLS, logits, -jnp.inf)
    shifted = logits - jnp.max(logits, axis=0, keepdims=True)
    log_prob = shifted - jnp.log(jnp.sum(jnp.exp(shifted), axis=0, keepdims=True))
    hit = classes == y_ref[...]
    weight = m_ref[...].astype(F32)
    picked = jnp.sum(jnp.where(hit, log_prob, 0.0), axis=0, keepdims=True)
    loss_part = -jnp.sum(weight * picked)
    grad = weight * (jnp.exp(log_prob) - jnp.where(hit, 1.0, 0.0)) / label_count
    gt[...] = grad.astype(BF16)
    ut[...] = lax.dot_general(w2t[...], gt[...], TN, preferred_element_type=F32).astype(BF16)

    def pair_sum(mask):
        return remote(acc.at[8 + mask], drecv.at[mask], es.at[mask], er.at[mask], dev(0, 1))

    def unit_copy(part, k):
        axis, mask = reduce_unit(part, k)
        rows = pl.ds(*REDUCE_ROWS[part])
        n = part * 7 + k
        return remote(acc.at[mask, rows], rbuf.at[k, rows], rs.at[n], rr.at[n], dev(1 << axis))

    def add_rows(mask, source, start, size):
        @pl.loop(0, size // 8)
        def _(t):
            rows = pl.ds(pl.multiple_of(start + t * 8, 8), 8)
            acc[mask, rows, :] += source[rows, :]

    def take_pair(mask):
        pair_sum(mask).wait_recv()
        add_rows(mask, drecv.at[mask], 0, HID)
        for k in range(4):
            for part in range(3):
                if reduce_unit(part, k)[1] == mask:
                    unit_copy(part, k).start()

    @pl.loop(0, NDEV)
    def _(i):
        slot = (NDEV - 1 - i) % RING
        mask, other = step_order(NDEV - 1 - i)

        @pl.when(i >= RING)
        def _():
            wait_a(slot)

        @pl.loop(0, 2)
        def _(half):
            cols = pl.ds(pl.multiple_of(half * 512, 512), 512)
            acc[mask + 8 * other, :, cols] = jnp.dot(ut[...], abuf[slot, :, cols], preferred_element_type=F32)

        @pl.when(i < NDEV - RING)
        def _():
            load_a(NDEV - 1 - i - RING, slot).start()

        for step in range(NDEV):
            step_mask, step_other = step_order(NDEV - 1 - step)

            @pl.when(i == step)
            def _():
                if step_other:
                    pair_sum(step_mask).start()
                else:
                    take_pair(step_mask)

    def small_scatter(src, dst, d, base, wait):
        if wait:
            ref = dst.at[peer(d)]
            return remote(ref, ref, ps.at[base + d], pr.at[base + d], peer(d))
        return remote(src.at[peer(d)], dst.at[me], ps.at[base + d], pr.at[base + d], peer(d))

    def small_gather(dst, d, base, wait):
        ref = dst.at[peer(d)] if wait else dst.at[me]
        return remote(ref, ref, ps.at[base + d], pr.at[base + d], peer(d))

    dw2_part = jnp.dot(gt[...], s2b[...], preferred_element_type=F32)
    d2src[...] = jnp.zeros_like(d2src)
    for j in range(6):
        d2src[j] = dw2_part[j * 8:(j + 1) * 8, 0:128]
        d2src[6 + j] = dw2_part[j * 8:(j + 1) * 8, 128:256]
    d2src[12] = jnp.full((8, 128), loss_part, F32)
    d2r1[me] = d2src[me]
    for d in far_first:
        small_scatter(d2src, d2r1, d, 0, False).start()

    def take_unit(part, k, send=None):
        axis, mask = reduce_unit(part, k)
        unit_copy(part, k).wait_recv()
        add_rows(mask - (1 << axis), rbuf.at[k], *REDUCE_ROWS[part])
        if send is not None:
            unit_copy(part, send).start()

    for part in range(3):
        take_unit(part, 0, 4)
    for part in range(3):
        take_unit(part, 1, 5)
    for part in range(3):
        take_unit(part, 2)
    for d in range(1, NDEV):
        small_scatter(d2src, d2r1, d, 0, True).wait_recv()
    d2r2[me] = jnp.sum(d2r1[...], axis=0)
    for d in far_first:
        small_gather(d2r2, d, 16, False).start()
    for part in range(3):
        take_unit(part, 3)
    for part in range(3):
        take_unit(part, 4, 6)
    for part in range(3):
        take_unit(part, 5)
    for part in range(3):
        take_unit(part, 6)

    grad_one = jnp.where(z1t[...] > 0.0, acc[0], 0.0).astype(BF16)
    d1src[...] = lax.dot_general(grad_one, s1b[...], NT, preferred_element_type=F32).reshape(NDEV, 16, FPAD)
    d1r1[me] = d1src[me]
    for d in far_first:
        small_scatter(d1src, d1r1, d, 32, False).start()
    for d in range(1, NDEV):
        small_gather(d2r2, d, 16, True).wait_recv()
    left = d2r2[0:6].reshape(CPAD, 128)
    right = d2r2[6:12].reshape(CPAD, 128)
    dw2_ref[...] = jnp.concatenate([left, right], axis=1)
    loss_ref[...] = d2r2[12] / label_count
    for d in range(1, NDEV):
        small_scatter(d1src, d1r1, d, 32, True).wait_recv()
    d1r2[me] = jnp.sum(d1r1[...], axis=0)
    for d in far_first:
        small_gather(d1r2, d, 48, False).start()
    drain_x()
    drain_h()
    for mask in range(8):
        pair_sum(mask).wait_send()
    for part in range(3):
        for k in range(7):
            unit_copy(part, k).wait_send()
    for d in range(1, NDEV):
        count_copy(d).wait_send()
        small_scatter(d2src, d2r1, d, 0, False).wait_send()
        small_gather(d2r2, d, 16, False).wait_send()
        small_scatter(d1src, d1r1, d, 32, False).wait_send()
    for d in range(1, NDEV):
        small_gather(d1r2, d, 48, True).wait_recv()
    dw1_ref[...] = d1r2[...].reshape(HID, FPAD)
    for d in range(1, NDEV):
        small_gather(d1r2, d, 48, False).wait_send()


def finish(loss_ref, dw1_ref, dw2_ref, loss_out, dw1_out, dw2_out):
    loss_out[...] = loss_ref[0:1, 0:1]
    dw1_out[...] = dw1_ref[...].T[0:FIN, :]
    dw2_out[...] = dw2_ref[0:NCLS, :]


def solution(mesh):
    def local_step(adj_rows, feat_rows, w_one, w_two, label_rows, mask_rows):
        vmem = pl.BlockSpec(memory_space=pltpu.VMEM)
        hbm = pl.BlockSpec(memory_space=pl.ANY)
        dma = pltpu.SemaphoreType.DMA
        parts = pl.pallas_call(
            kernel,
            out_shape=(jax.ShapeDtypeStruct((8, 128), F32), jax.ShapeDtypeStruct((HID, FPAD), F32),
                       jax.ShapeDtypeStruct((CPAD, HID), F32)),
            in_specs=[hbm] * 6,
            out_specs=(vmem, vmem, vmem),
            scratch_shapes=[
                pltpu.VMEM((RING, BLK, BLK), BF16),
                pltpu.VMEM((FIN, BLK), BF16),
                pltpu.VMEM((FIN, HID), F32),
                pltpu.VMEM((NCLS, HID), F32),
                pltpu.VMEM((1, BLK), jnp.int32),
                pltpu.VMEM((1, BLK), jnp.int32),
                pltpu.VMEM((NDEV, FROWS, BLK), BF16),
                pltpu.VMEM((NDEV, BLK, HID), BF16),
                pltpu.VMEM((FPAD, BLK), F32),
                pltpu.VMEM((BLK, HID), F32),
                pltpu.VMEM((FPAD, BLK), BF16),
                pltpu.VMEM((BLK, HID), BF16),
                pltpu.VMEM((HID, BLK), F32),
                pltpu.VMEM((FPAD, HID), F32),
                pltpu.VMEM((HID, FPAD), BF16),
                pltpu.VMEM((CPAD, HID), BF16),
                pltpu.VMEM((HID, BLK), BF16),
                pltpu.VMEM((16, HID, BLK), F32),
                pltpu.VMEM((8, HID, BLK), F32),
                pltpu.VMEM((7, HID, BLK), F32),
                pltpu.VMEM((CPAD, BLK), BF16),
                pltpu.VMEM((NDEV, 8, 128), F32),
                pltpu.VMEM((NDEV, 8, 128), F32),
                pltpu.VMEM((NDEV, 8, 128), F32),
                pltpu.VMEM((NDEV, 8, 128), F32),
                pltpu.VMEM((NDEV, 16, FPAD), F32),
                pltpu.VMEM((NDEV, 16, FPAD), F32),
                pltpu.VMEM((NDEV, 16, FPAD), F32),
                dma((RING,)), dma((5,)), dma((42,)), dma((42,)), dma((16,)), dma((16,)), dma((21,)), dma((21,)),
                dma((8,)), dma((8,)), dma((16,)), dma((16,)), dma((64,)), dma((64,)),
            ],
            compiler_params=pltpu.CompilerParams(collective_id=0, has_side_effects=True,
                                                 vmem_limit_bytes=62 * 1000 * 1000),
        )(adj_rows, feat_rows.T, w_one, w_two.T, label_rows.reshape(1, BLK), mask_rows.reshape(1, BLK))
        loss, dw_one, dw_two = pl.pallas_call(
            finish,
            out_shape=(jax.ShapeDtypeStruct((1, 1), F32), jax.ShapeDtypeStruct((FIN, HID), F32),
                       jax.ShapeDtypeStruct((NCLS, HID), F32)),
            in_specs=[vmem] * 3,
            out_specs=(vmem, vmem, vmem),
        )(*parts)
        return loss.reshape(1), dw_one, dw_two.T

    return jax.shard_map(local_step, mesh=mesh,
                         in_specs=(P(AXIS, None), P(AXIS, None), P(None, None), P(None, None), P(AXIS), P(AXIS)),
                         out_specs=(P(None), P(None, None), P(None, None)), check_vma=False)
```

```python
import functools

import jax
import jax.numpy as jnp
from jax import lax
from jax.experimental import pallas as pl
from jax.experimental.pallas import tpu as pltpu
from jax.sharding import PartitionSpec as P

MESH = pl.DeviceIdType.MESH
AXIS = 'nodes'
F32, BF16 = jnp.float32, jnp.bfloat16
NDEV = 16
BLK = 1024
FIN, FROWS, FPAD = 100, 104, 128
HID = 256
NCLS, CPAD = 47, 48
RING = 6
SEMS = 64
TILE = (8, 128)

ORDER = tuple((p, (p + 1) % 3, (p + 2) % 3) for p in range(3))
GATHER_ROWS = ((0, 352), (352, 336), (688, 336))
GATHER_COLS = ((0, 384), (384, 384), (768, 256))
REDUCE_ROWS = ((0, 88), (88, 88), (176, 80))

NT = (((1,), (1,)), ((), ()))
TN = (((0,), (0,)), ((), ()))


def gather_unit(axis, slot):
    first, second, third = axis, (axis + 2) % 3, (axis + 1) % 3
    if slot == 0:
        return first, 0
    if slot == 1:
        return second, 0
    if slot == 2:
        return third, 0
    if slot == 3:
        return second, 1 << ORDER[second][0]
    one, two = 1 << ORDER[third][0], 1 << ORDER[third][1]
    return third, {4: one, 5: two, 6: one | two}[slot]


def reduce_unit(part, k):
    b1, b2, b3 = ORDER[part]
    m1, m2, m3 = 1 << b1, 1 << b2, 1 << b3
    return ((b1, m1 | m2 | m3), (b1, m1 | m2), (b1, m1 | m3), (b1, m1), (b2, m2 | m3), (b2, m2), (b3, m3))[k]


def step_order(i):
    from2, from8, from10, from14 = ((i + 16 - n) // 16 for n in (2, 8, 10, 14))
    j = (i + 1) % 3
    one, xy, two = from2 - from8, from8 - from10, from10 - from14
    mask = one * ((j * j + j + 2) // 2) + xy * 3 + two * (5 + i % 2) + from14 * 7
    core = (1 - from2) * i + one * ((i + 1) // 3 - 1) + xy * (i - 8) + two * (i // 2 - 5) + from14 * (i - 14)
    return mask, core


def flip(bit, by):
    return bit + by - 2 * bit * by


def kernel(a_hbm, x_hbm, w1_hbm, w2_hbm, y_hbm, m_hbm, loss_ref, dw1_ref, dw2_ref,
           abuf, xin, w1_ref, w2_ref, y_ref, m_ref, xall, hall, s1acc, s2acc, s1b, s2b, z1t, w1p, w1t, w2t, ut,
           acc, drecv, rbuf, gt,
           cnt, d2src, d2r1, d2r2, d1src, d1r1, d1r2,
           asem, xsem, gs, gr, ds, dr, rs, rr, es, er, ms, mr, ps, pr):
    me = lax.axis_index(AXIS)
    core, px, py, pz = me % 2, (me // 2) % 2, (me // 4) % 2, me // 8

    def dev(mask, other=0):
        fx, fy, fz, fc = mask % 2, (mask // 2) % 2, mask // 4, other
        return ((flip(pz, fz) * 2 + flip(py, fy)) * 2 + flip(px, fx)) * 2 + flip(core, fc)

    def block_of(i):
        mask, other = step_order(i)
        return dev(mask, other)

    def load_a(i, slot):
        start = pl.multiple_of(block_of(i) * BLK, BLK)
        return pltpu.make_async_copy(a_hbm.at[:, pl.ds(start, BLK)], abuf.at[slot], asem.at[slot])

    def wait_a(slot):
        pltpu.make_async_copy(a_hbm.at[:, pl.ds(0, BLK)], abuf.at[slot], asem.at[slot]).wait()

    def remote(src, dst, send, recv, to):
        return pltpu.make_async_remote_copy(src_ref=src, dst_ref=dst, send_sem=send, recv_sem=recv,
                                            device_id=(to,), device_id_type=MESH)

    def peer(d):
        return dev(d // 2, d % 2)

    far_first = sorted(range(1, NDEV), key=lambda d: -bin(d // 2).count('1'))

    loads = [pltpu.make_async_copy(src, dst, xsem.at[k]) for k, (src, dst) in enumerate((
        (x_hbm, xin), (m_hbm, m_ref), (w1_hbm, w1_ref), (w2_hbm, w2_ref), (y_hbm, y_ref)))]
    for load in loads:
        load.start()
    for i in range(RING):
        load_a(i, i).start()
    barrier = pltpu.get_barrier_semaphore()
    for d in (8, 4, 2, 1):
        pl.semaphore_signal(barrier, inc=1, device_id=(peer(d),), device_id_type=MESH)
    xall[me] = jnp.zeros((FROWS, BLK), BF16)
    loads[0].wait()
    xall[me, 0:FIN, :] = xin[...]
    loads[1].wait()
    cnt[me] = jnp.full((1, 128), jnp.sum(m_ref[...].astype(F32)), F32)
    pl.semaphore_wait(barrier, 4)

    def gather(buf, g):
        def piece(owner, part):
            return buf.at[owner, :, pl.ds(*GATHER_COLS[part])] if g == 0 else buf.at[owner, pl.ds(*GATHER_ROWS[part])]

        def copy(axis, slot, at_receiver=False):
            part, mask = gather_unit(axis, slot)
            owner = dev(mask | (1 << axis) if at_receiver else mask)
            ref = piece(owner, part)
            n = g * 21 + axis * 7 + slot
            return remote(ref, ref, gs.at[n], gr.at[n], dev(1 << axis))

        def pair(mask, at_receiver=False):
            return [pair_piece(mask, k, at_receiver) for k in range(1 if mask < 7 else 3)]

        def pair_piece(mask, k, at_receiver=False):
            owner = dev(mask, 1 if at_receiver else 0)
            ref = buf.at[owner] if mask < 7 else piece(owner, k)
            return remote(ref, ref, ds.at[g * 10 + mask + k], dr.at[g * 10 + mask + k], dev(0, 1))

        def give(*masks):
            for mask in masks:
                for c in pair(mask):
                    c.start()

        def take(mask):
            for c in pair(mask, True):
                c.wait_recv()

        def begin():
            for slot in range(3):
                for axis in range(3):
                    copy(axis, slot).start()
            give(0)

        def arrive(*arrivals):
            for axis, slot in arrivals:
                copy(axis, slot, True).wait_recv()
                part, mask = gather_unit(axis, slot)
                got = (part, mask | (1 << axis))
                for later in (3, 4, 5, 6):
                    for onto in range(3):
                        if gather_unit(onto, later) == got and not (onto == 1 and later == 4):
                            copy(onto, later).start()
                if slot == 1 and axis == gather_unit_source():
                    copy(1, 4).start()

        def gather_unit_source():
            return next(a for a in range(3) if gather_unit(1, 5) == (gather_unit(a, 1)[0], 1 << a))

        def hooks(p):
            @pl.when(p == 0)
            def _():
                take(0)

            @pl.when(p == 1)
            def _():
                arrive(*((axis, slot) for slot in range(3) for axis in range(3)))
                give(1, 2, 4)

            @pl.when(p == 2)
            def _():
                take(1)

            @pl.when(p == 3)
            def _():
                take(2)
                take(4)

            @pl.when(p == 4)
            def _():
                arrive((0, 3), (1, 3), (2, 3), (1, 5), (0, 4))
                give(3)
                take(3)

            @pl.when(p == 5)
            def _():
                arrive((2, 4), (1, 4), (0, 5), (2, 5))
                give(5, 6)

            @pl.when(p == 6)
            def _():
                take(5)
                take(6)

        def tail(i):
            @pl.when(i == 0)
            def _():
                for part in range(3):
                    arrive(((part + 2) % 3, 6))
                    pair_piece(7, part).start()

            @pl.when(i == 1)
            def _():
                take(7)

        def drain():
            for axis in range(3):
                for slot in range(7):
                    copy(axis, slot).wait_send()
            for mask in range(8):
                for c in pair(mask):
                    c.wait_send()

        return begin, hooks, tail, drain

    def aggregate(buf, total, hooks, tail, g):
        def product(i):
            slot = (16 * g + i) % RING
            if g == 0:
                return lax.dot_general(buf[block_of(i)], abuf[slot], NT, preferred_element_type=F32)
            return jnp.dot(abuf[slot], buf[block_of(i)], preferred_element_type=F32)

        def refill(i):
            slot = (16 * g + i) % RING
            if g == 0:
                load_a((i + RING) % NDEV, slot).start()
            else:
                @pl.when(i < NDEV - RING)
                def _():
                    load_a(i + RING, slot).start()

        rows = pl.ds(0, FROWS if g == 0 else BLK)

        @pl.loop(0, 7)
        def _(p):
            hooks(p)
            wait_a((16 * g + 2 * p) % RING)
            wait_a((16 * g + 2 * p + 1) % RING)
            total[rows, :] += product(2 * p) + product(2 * p + 1)
            refill(2 * p)
            refill(2 * p + 1)

        @pl.loop(0, 2)
        def _(k):
            tail(k)
            wait_a((16 * g + 14 + k) % RING)
            total[rows, :] += product(14 + k)
            refill(14 + k)

    def count_copy(d):
        ref = cnt.at[me]
        return remote(ref, ref, ms.at[d], mr.at[d], peer(d))

    begin_x, hooks_x, tail_x, drain_x = gather(xall, 0)
    begin_h, hooks_h, tail_h, drain_h = gather(hall, 1)

    begin_x()
    for load in loads[2:]:
        load.wait()
    w1p[...] = jnp.zeros_like(w1p)
    w1p[0:FIN, :] = w1_ref[...]
    w1t[...] = w1p[...].T.astype(BF16)
    w2t[...] = jnp.zeros_like(w2t)
    w2t[0:NCLS, :] = w2_ref[...].astype(BF16)
    s1acc[...] = jnp.zeros_like(s1acc)
    s2acc[...] = jnp.zeros_like(s2acc)
    aggregate(xall, s1acc, hooks_x, tail_x, 0)

    s1b[...] = s1acc[...].astype(BF16)
    pre_one = jnp.dot(s1acc[...].T.astype(BF16), w1p[...].astype(BF16), preferred_element_type=F32)
    hall[me] = jnp.maximum(pre_one, 0.0).astype(BF16)
    begin_h()
    for d in far_first:
        count_copy(d).start()
    z1t[...] = jnp.dot(w1t[...], s1b[...], preferred_element_type=F32)
    aggregate(hall, s2acc, hooks_h, tail_h, 1)

    for d in range(1, NDEV):
        ref = cnt.at[peer(d)]
        remote(ref, ref, ms.at[d], mr.at[d], peer(d)).wait_recv()
    label_count = jnp.sum(cnt[...], axis=0)[0:1, 0:1]
    s2b[...] = s2acc[...].astype(BF16)
    logits = lax.dot_general(w2t[...], s2b[...], NT, preferred_element_type=F32)
    classes = lax.broadcasted_iota(jnp.int32, (CPAD, BLK), 0)
    logits = jnp.where(classes < NCLS, logits, -jnp.inf)
    shifted = logits - jnp.max(logits, axis=0, keepdims=True)
    log_prob = shifted - jnp.log(jnp.sum(jnp.exp(shifted), axis=0, keepdims=True))
    hit = classes == y_ref[...]
    weight = m_ref[...].astype(F32)
    picked = jnp.sum(jnp.where(hit, log_prob, 0.0), axis=0, keepdims=True)
    loss_part = -jnp.sum(weight * picked)
    grad = weight * (jnp.exp(log_prob) - jnp.where(hit, 1.0, 0.0)) / label_count
    gt[...] = grad.astype(BF16)
    ut[...] = lax.dot_general(w2t[...], gt[...], TN, preferred_element_type=F32).astype(BF16)

    def pair_sum(mask, half=None):
        if half is None:
            return remote(acc.at[8 + mask], drecv.at[mask], es.at[mask], er.at[mask], dev(0, 1))
        cols = pl.ds(half * 512, 512)
        return remote(acc.at[8 + mask, :, cols], drecv.at[mask, :, cols], es.at[mask + half], er.at[mask + half],
                      dev(0, 1))

    def unit_copy(part, k, half=None):
        axis, mask = reduce_unit(part, k)
        rows = pl.ds(*REDUCE_ROWS[part])
        n = part * 7 + k
        if half is None:
            return remote(acc.at[mask, rows], rbuf.at[k, rows], rs.at[n], rr.at[n], dev(1 << axis))
        cols = pl.ds(half * 512, 512)
        n = n if half == 0 else 21 + part
        return remote(acc.at[mask, rows, cols], rbuf.at[k, rows, cols], rs.at[n], rr.at[n], dev(1 << axis))

    def unit_copies(part, k):
        return [unit_copy(part, k, half) for half in ((0, 1) if k == 0 else (None,))]

    def add_rows(mask, source, start, size, cols=slice(None)):
        @pl.loop(0, size // 8)
        def _(t):
            rows = pl.ds(pl.multiple_of(start + t * 8, 8), 8)
            acc[mask, rows, cols] += source[rows, cols]

    def take_pair(mask):
        pair_sum(mask).wait_recv()
        add_rows(mask, drecv.at[mask], 0, HID)
        for k in range(1, 4):
            for part in range(3):
                if reduce_unit(part, k)[1] == mask:
                    unit_copy(part, k).start()

    def small_scatter(src, dst, d, base, wait):
        if wait:
            ref = dst.at[peer(d)]
            return remote(ref, ref, ps.at[base + d], pr.at[base + d], peer(d))
        return remote(src.at[peer(d)], dst.at[me], ps.at[base + d], pr.at[base + d], peer(d))

    def small_gather(dst, d, base, wait):
        ref = dst.at[peer(d)] if wait else dst.at[me]
        return remote(ref, ref, ps.at[base + d], pr.at[base + d], peer(d))

    @pl.loop(0, 4)
    def _(q):
        other, half = 1 - q // 2, q % 2
        cols = pl.ds(pl.multiple_of(half * 512, 512), 512)
        acc[7 + 8 * other, :, cols] = jnp.dot(ut[...], abuf[(30 + other) % RING, :, cols], preferred_element_type=F32)
        for half in range(2):
            @pl.when(q == half)
            def _():
                pair_sum(7, half).start()

    for j in range(2):
        load_a(NDEV - 1 - j - RING, (31 - j) % RING).start()

    dw2_part = jnp.dot(gt[...], s2b[...], preferred_element_type=F32)
    d2src[...] = jnp.zeros_like(d2src)
    for j in range(6):
        for k in range(2):
            d2src[6 * k + j] = dw2_part[j * 8:(j + 1) * 8, k * 128:(k + 1) * 128]
    d2src[12] = jnp.full(TILE, loss_part, F32)
    d2r1[me] = d2src[me]
    for d in far_first:
        small_scatter(d2src, d2r1, d, 0, False).start()

    for half in range(2):
        pair_sum(7, half).wait_recv()
        add_rows(7, drecv.at[7], 0, HID, pl.ds(half * 512, 512))
        for part in range(3):
            unit_copy(part, 0, half).start()

    @pl.loop(1, 8)
    def _(p):
        for k in range(2):
            @pl.when(p >= 3)
            def _():
                wait_a((31 - 2 * p - k) % RING)
        for k in range(2):
            mask, other = step_order(NDEV - 1 - 2 * p - k)
            acc[mask + 8 * other] = jnp.dot(ut[...], abuf[(31 - 2 * p - k) % RING], preferred_element_type=F32)
        for k in range(2):
            @pl.when(p < 5)
            def _():
                load_a(NDEV - 1 - 2 * p - k - RING, (31 - 2 * p - k) % RING).start()

        for step in range(2, NDEV):
            step_mask, step_other = step_order(NDEV - 1 - step)

            @pl.when(p == step // 2)
            def _():
                if step_other:
                    pair_sum(step_mask).start()
                else:
                    take_pair(step_mask)

    def take_unit(part, k, send=None):
        axis, mask = reduce_unit(part, k)
        for c in unit_copies(part, k):
            c.wait_recv()
        add_rows(mask - (1 << axis), rbuf.at[k], *REDUCE_ROWS[part])
        if send is not None:
            unit_copy(part, send).start()

    for k in range(2):
        for part in range(3):
            take_unit(part, k, k + 4)
    for part in range(3):
        take_unit(part, 2)
    for d in range(1, NDEV):
        small_scatter(d2src, d2r1, d, 0, True).wait_recv()
    d2r2[me] = jnp.sum(d2r1[...], axis=0)
    for part in range(3):
        take_unit(part, 3)
    for part in range(3):
        take_unit(part, 4, 6)
    for d in far_first:
        small_gather(d2r2, d, 16, False).start()
    for k in (5, 6):
        for part in range(3):
            take_unit(part, k)

    grad_one = jnp.where(z1t[...] > 0.0, acc[0], 0.0).astype(BF16)
    d1src[...] = lax.dot_general(grad_one, s1b[...], NT, preferred_element_type=F32).reshape(NDEV, 16, FPAD)
    d1r1[me] = d1src[me]
    for d in far_first:
        small_scatter(d1src, d1r1, d, 32, False).start()
    for d in range(1, NDEV):
        small_gather(d2r2, d, 16, True).wait_recv()
    for k in range(2):
        dw2_ref[:, pl.ds(k * 128, 128)] = d2r2[pl.ds(6 * k, 6)].reshape(CPAD, 128)
    loss_ref[...] = d2r2[12] / label_count
    for d in range(1, NDEV):
        small_scatter(d1src, d1r1, d, 32, True).wait_recv()
    d1r2[me] = jnp.sum(d1r1[...], axis=0)
    for d in far_first:
        small_gather(d1r2, d, 48, False).start()
    drain_x()
    drain_h()
    for mask in range(7):
        pair_sum(mask).wait_send()
    for half in range(2):
        pair_sum(7, half).wait_send()
    for part in range(3):
        for k in range(7):
            for c in unit_copies(part, k):
                c.wait_send()
    for d in range(1, NDEV):
        count_copy(d).wait_send()
        small_scatter(d2src, d2r1, d, 0, False).wait_send()
        small_gather(d2r2, d, 16, False).wait_send()
        small_scatter(d1src, d1r1, d, 32, False).wait_send()
    for d in range(1, NDEV):
        small_gather(d1r2, d, 48, True).wait_recv()
    dw1_ref[...] = d1r2[...].reshape(HID, FPAD)
    for d in range(1, NDEV):
        small_gather(d1r2, d, 48, False).wait_send()


def finish(loss_ref, dw1_ref, dw2_ref, loss_out, dw1_out, dw2_out):
    loss_out[...] = loss_ref[0:1, 0:1]
    dw1_out[...] = dw1_ref[...].T[0:FIN, :]
    dw2_out[...] = dw2_ref[0:NCLS, :]


def solution(mesh):
    def local_step(adj_rows, feat_rows, w_one, w_two, label_rows, mask_rows):
        vmem = pl.BlockSpec(memory_space=pltpu.VMEM)
        hbm = pl.BlockSpec(memory_space=pl.ANY)
        dma = pltpu.SemaphoreType.DMA
        parts = pl.pallas_call(
            kernel,
            out_shape=(jax.ShapeDtypeStruct(TILE, F32), jax.ShapeDtypeStruct((HID, FPAD), F32),
                       jax.ShapeDtypeStruct((CPAD, HID), F32)),
            in_specs=[hbm] * 6,
            out_specs=(vmem, vmem, vmem),
            scratch_shapes=[
                pltpu.VMEM((RING, BLK, BLK), BF16),
                pltpu.VMEM((FIN, BLK), BF16),
                pltpu.VMEM((FIN, HID), F32),
                pltpu.VMEM((NCLS, HID), F32),
                pltpu.VMEM((1, BLK), jnp.int32),
                pltpu.VMEM((1, BLK), jnp.int32),
                pltpu.VMEM((NDEV, FROWS, BLK), BF16),
                pltpu.VMEM((NDEV, BLK, HID), BF16),
                pltpu.VMEM((FPAD, BLK), F32),
                pltpu.VMEM((BLK, HID), F32),
                pltpu.VMEM((FPAD, BLK), BF16),
                pltpu.VMEM((BLK, HID), BF16),
                pltpu.VMEM((HID, BLK), F32),
                pltpu.VMEM((FPAD, HID), F32),
                pltpu.VMEM((HID, FPAD), BF16),
                pltpu.VMEM((CPAD, HID), BF16),
                pltpu.VMEM((HID, BLK), BF16),
                pltpu.VMEM((16, HID, BLK), F32),
                pltpu.VMEM((8, HID, BLK), F32),
                pltpu.VMEM((7, HID, BLK), F32),
                pltpu.VMEM((CPAD, BLK), BF16),
                pltpu.VMEM((NDEV, 1, 128), F32),
                *[pltpu.VMEM((NDEV, *TILE), F32)] * 3,
                *[pltpu.VMEM((NDEV, 16, FPAD), F32)] * 3,
                *[dma((SEMS,))] * 14,
            ],
            compiler_params=pltpu.CompilerParams(collective_id=0, has_side_effects=True,
                                                 vmem_limit_bytes=67 * 1000 * 1000),
        )(adj_rows, feat_rows.T, w_one, w_two.T, label_rows.reshape(1, BLK), mask_rows.reshape(1, BLK))
        loss, dw_one, dw_two = pl.pallas_call(
            finish,
            out_shape=(jax.ShapeDtypeStruct((1, 1), F32), jax.ShapeDtypeStruct((FIN, HID), F32),
                       jax.ShapeDtypeStruct((NCLS, HID), F32)),
            in_specs=[vmem] * 3,
            out_specs=(vmem, vmem, vmem),
        )(*parts)
        return loss.reshape(1), dw_one, dw_two.T

    return jax.shard_map(local_step, mesh=mesh,
                         in_specs=(P(AXIS, None), P(AXIS, None), P(None, None), P(None, None), P(AXIS), P(AXIS)),
                         out_specs=(P(None), P(None, None), P(None, None)), check_vma=False)
```

```python
import functools

import jax
import jax.numpy as jnp
from jax import lax
from jax.experimental import pallas as pl
from jax.experimental.pallas import tpu as pltpu
from jax.sharding import PartitionSpec as P

MESH = pl.DeviceIdType.MESH
AXIS = 'nodes'
F32, BF16 = jnp.float32, jnp.bfloat16
NDEV = 16
BLK = 1024
FIN, FROWS, FPAD = 100, 104, 128
HID = 256
NCLS, CPAD = 47, 48
RING = 6
TILE = (8, 128)

ORDER = tuple((p, (p + 1) % 3, (p + 2) % 3) for p in range(3))
GATHER_ROWS = ((0, 352), (352, 336), (688, 336))
GATHER_COLS = ((0, 384), (384, 384), (768, 256))
REDUCE_ROWS = ((0, 88), (88, 88), (176, 80))

NT = (((1,), (1,)), ((), ()))
TN = (((0,), (0,)), ((), ()))


def gather_unit(axis, slot):
    first, second, third = axis, (axis + 2) % 3, (axis + 1) % 3
    if slot == 0:
        return first, 0
    if slot == 1:
        return second, 0
    if slot == 2:
        return third, 0
    if slot == 3:
        return second, 1 << ORDER[second][0]
    one, two = 1 << ORDER[third][0], 1 << ORDER[third][1]
    return third, {4: one, 5: two, 6: one | two}[slot]


def reduce_unit(part, k):
    b1, b2, b3 = ORDER[part]
    m1, m2, m3 = 1 << b1, 1 << b2, 1 << b3
    return ((b1, m1 | m2 | m3), (b1, m1 | m2), (b1, m1 | m3), (b1, m1), (b2, m2 | m3), (b2, m2), (b3, m3))[k]


def step_order(i):
    from2, from8, from10, from14 = ((i + 16 - n) // 16 for n in (2, 8, 10, 14))
    j = (i + 1) % 3
    one, xy, two = from2 - from8, from8 - from10, from10 - from14
    mask = one * ((j * j + j + 2) // 2) + xy * 3 + two * (5 + i % 2) + from14 * 7
    core = (1 - from2) * i + one * ((i + 1) // 3 - 1) + xy * (i - 8) + two * (i // 2 - 5) + from14 * (i - 14)
    return mask, core


def flip(bit, by):
    return bit + by - 2 * bit * by


def kernel(a_hbm, x_hbm, w1_hbm, w2_hbm, y_hbm, m_hbm, d1out, d2out,
           abuf, xin, w1_ref, w2_ref, y_ref, m_ref, xall, hall, s1acc, s2acc, s1b, s2b, z1t, w1p, w1t, w2t, ut,
           acc, drecv, rbuf, gt,
           cnt, d2src, d2r1, d2r2, d1src, d1r1, d1r2,
           asem, xsem, gr, dr, rr, er, pr, snd):
    me = lax.axis_index(AXIS)
    core, px, py, pz = me % 2, (me // 2) % 2, (me // 4) % 2, me // 8

    def dev(mask, other=0):
        fx, fy, fz, fc = mask % 2, (mask // 2) % 2, mask // 4, other
        return ((flip(pz, fz) * 2 + flip(py, fy)) * 2 + flip(px, fx)) * 2 + flip(core, fc)

    def block_of(i):
        mask, other = step_order(i)
        return dev(mask, other)

    def load_a(i, slot):
        start = pl.multiple_of(block_of(i) * BLK, BLK)
        return pltpu.make_async_copy(a_hbm.at[:, pl.ds(start, BLK)], abuf.at[slot], asem.at[slot])

    def wait_a(slot):
        pltpu.make_async_copy(a_hbm.at[:, pl.ds(0, BLK)], abuf.at[slot], asem.at[slot]).wait()

    def remote(src, dst, send, recv, to):
        return pltpu.make_async_remote_copy(src_ref=src, dst_ref=dst, send_sem=send, recv_sem=recv,
                                            device_id=(to,), device_id_type=MESH)

    def peer(d):
        return dev(d // 2, d % 2)

    far_first = sorted(range(1, NDEV), key=lambda d: -bin(d // 2).count('1'))

    loads = [pltpu.make_async_copy(src, dst, xsem.at[k]) for k, (src, dst) in enumerate((
        (x_hbm, xin), (m_hbm, m_ref), (w1_hbm, w1_ref), (w2_hbm, w2_ref), (y_hbm, y_ref)))]
    for load in loads:
        load.start()
    for i in range(RING):
        load_a(i, i).start()
    barrier = pltpu.get_barrier_semaphore()
    for d in (8, 4, 2, 1):
        pl.semaphore_signal(barrier, inc=1, device_id=(peer(d),), device_id_type=MESH)
    xall[me] = jnp.zeros((FROWS, BLK), BF16)
    loads[0].wait()
    xall[me, 0:FIN, :] = xin[...]
    loads[1].wait()
    cnt[me] = jnp.full((1, 128), jnp.sum(m_ref[...].astype(F32)), F32)
    pl.semaphore_wait(barrier, 4)

    def gather(buf, g):
        def piece(owner, part):
            return buf.at[owner, :, pl.ds(*GATHER_COLS[part])] if g == 0 else buf.at[owner, pl.ds(*GATHER_ROWS[part])]

        def copy(axis, slot, at_receiver=False):
            part, mask = gather_unit(axis, slot)
            owner = dev(mask | (1 << axis) if at_receiver else mask)
            ref = piece(owner, part)
            n = g * 21 + axis * 7 + slot
            return remote(ref, ref, snd.at[g], gr.at[n], dev(1 << axis))

        def pair(mask, at_receiver=False):
            return [pair_piece(mask, k, at_receiver) for k in range(1 if mask < 7 else 3)]

        def pair_piece(mask, k, at_receiver=False):
            owner = dev(mask, 1 if at_receiver else 0)
            ref = buf.at[owner] if mask < 7 else piece(owner, k)
            return remote(ref, ref, snd.at[g], dr.at[g * 10 + mask + k], dev(0, 1))

        def give(*masks):
            for mask in masks:
                for c in pair(mask):
                    c.start()

        def take(mask):
            for c in pair(mask, True):
                c.wait_recv()

        def begin():
            for slot in range(3):
                for axis in range(3):
                    copy(axis, slot).start()
            give(0)

        def arrive(*arrivals):
            for axis, slot in arrivals:
                copy(axis, slot, True).wait_recv()
                part, mask = gather_unit(axis, slot)
                got = (part, mask | (1 << axis))
                for later in (3, 4, 5, 6):
                    for onto in range(3):
                        if gather_unit(onto, later) == got and not (onto == 1 and later == 4):
                            copy(onto, later).start()
                if slot == 1 and axis == gather_unit_source():
                    copy(1, 4).start()

        def gather_unit_source():
            return next(a for a in range(3) if gather_unit(1, 5) == (gather_unit(a, 1)[0], 1 << a))

        def hooks(p):
            @pl.when(p == 0)
            def _():
                take(0)

            @pl.when(p == 1)
            def _():
                arrive(*((axis, slot) for slot in range(3) for axis in range(3)))
                give(1, 2, 4)

            @pl.when(p == 2)
            def _():
                take(1)

            @pl.when(p == 3)
            def _():
                take(2)
                take(4)

            @pl.when(p == 4)
            def _():
                arrive((0, 3), (1, 3), (2, 3), (1, 5), (0, 4))
                give(3)
                take(3)

            @pl.when(p == 5)
            def _():
                arrive((2, 4), (1, 4), (0, 5), (2, 5))
                give(5, 6)

            @pl.when(p == 6)
            def _():
                take(5)
                take(6)

        def tail(i):
            @pl.when(i == 0)
            def _():
                for part in range(3):
                    arrive(((part + 2) % 3, 6))
                    pair_piece(7, part).start()

            @pl.when(i == 1)
            def _():
                take(7)

        def drain():
            every = buf.at[pl.ds(0, 15)]
            remote(every, every, snd.at[g], gr.at[0], me).wait_send()

        return begin, hooks, tail, drain

    def aggregate(buf, total, hooks, tail, g):
        def product(i):
            slot = (16 * g + i) % RING
            if g == 0:
                return lax.dot_general(buf[block_of(i)], abuf[slot], NT, preferred_element_type=F32)
            return jnp.dot(abuf[slot], buf[block_of(i)], preferred_element_type=F32)

        def refill(i):
            slot = (16 * g + i) % RING
            if g == 0:
                load_a((i + RING) % NDEV, slot).start()
            else:
                @pl.when(i < NDEV - RING)
                def _():
                    load_a(i + RING, slot).start()

        rows = pl.ds(0, FROWS if g == 0 else BLK)

        @pl.loop(0, 7)
        def _(p):
            hooks(p)
            wait_a((16 * g + 2 * p) % RING)
            wait_a((16 * g + 2 * p + 1) % RING)
            total[rows, :] += product(2 * p) + product(2 * p + 1)
            refill(2 * p)
            refill(2 * p + 1)

        @pl.loop(0, 2)
        def _(k):
            tail(k)
            wait_a((16 * g + 14 + k) % RING)
            total[rows, :] += product(14 + k)
            refill(14 + k)

    def small(x, src, dst, scatter=False):
        for d in far_first:
            remote(src.at[peer(d)] if scatter else src, dst.at[me], snd.at[3 + x], pr.at[x], peer(d)).start()

    def small_wait(x, dst):
        ref = dst.at[pl.ds(0, 15)]
        remote(ref, ref, snd.at[3 + x], pr.at[x], me).wait()

    begin_x, hooks_x, tail_x, drain_x = gather(xall, 0)
    begin_h, hooks_h, tail_h, drain_h = gather(hall, 1)

    begin_x()
    for load in loads[2:]:
        load.wait()
    w1p[...] = jnp.zeros_like(w1p)
    w1p[0:FIN, :] = w1_ref[...]
    w1t[...] = w1p[...].T.astype(BF16)
    w2t[...] = jnp.zeros_like(w2t)
    w2t[0:NCLS, :] = w2_ref[...].astype(BF16)
    s1acc[...] = jnp.zeros_like(s1acc)
    s2acc[...] = jnp.zeros_like(s2acc)
    aggregate(xall, s1acc, hooks_x, tail_x, 0)

    s1b[...] = s1acc[...].astype(BF16)
    pre_one = jnp.dot(s1acc[...].T.astype(BF16), w1p[...].astype(BF16), preferred_element_type=F32)
    hall[me] = jnp.maximum(pre_one, 0.0).astype(BF16)
    begin_h()
    small(0, cnt.at[me], cnt)
    z1t[...] = jnp.dot(w1t[...], s1b[...], preferred_element_type=F32)
    aggregate(hall, s2acc, hooks_h, tail_h, 1)

    small_wait(0, cnt)
    label_count = jnp.sum(cnt[...], axis=0)[0:1, 0:1]
    s2b[...] = s2acc[...].astype(BF16)
    logits = lax.dot_general(w2t[...], s2b[...], NT, preferred_element_type=F32)
    classes = lax.broadcasted_iota(jnp.int32, (CPAD, BLK), 0)
    logits = jnp.where(classes < NCLS, logits, -jnp.inf)
    shifted = logits - jnp.max(logits, axis=0, keepdims=True)
    log_prob = shifted - jnp.log(jnp.sum(jnp.exp(shifted), axis=0, keepdims=True))
    hit = classes == y_ref[...]
    weight = m_ref[...].astype(F32)
    picked = jnp.sum(jnp.where(hit, log_prob, 0.0), axis=0, keepdims=True)
    loss_part = -jnp.sum(weight * picked)
    grad = weight * (jnp.exp(log_prob) - jnp.where(hit, 1.0, 0.0)) / label_count
    gt[...] = grad.astype(BF16)
    ut[...] = lax.dot_general(w2t[...], gt[...], TN, preferred_element_type=F32).astype(BF16)

    def pair_sum(mask, half=None):
        if half is None:
            return remote(acc.at[8 + mask], drecv.at[mask], snd.at[2], er.at[mask], dev(0, 1))
        cols = pl.ds(half * 512, 512)
        return remote(acc.at[8 + mask, :, cols], drecv.at[mask, :, cols], snd.at[2], er.at[mask + half],
                      dev(0, 1))

    def unit_copy(part, k, half=None):
        axis, mask = reduce_unit(part, k)
        rows = pl.ds(*REDUCE_ROWS[part])
        n = part * 7 + k
        if half is None:
            return remote(acc.at[mask, rows], rbuf.at[k, rows], snd.at[2], rr.at[n], dev(1 << axis))
        cols = pl.ds(half * 512, 512)
        n = n if half == 0 else 21 + part
        return remote(acc.at[mask, rows, cols], rbuf.at[k, rows, cols], snd.at[2], rr.at[n], dev(1 << axis))

    def unit_copies(part, k):
        return [unit_copy(part, k, half) for half in ((0, 1) if k == 0 else (None,))]

    def add_rows(mask, source, start, size, cols=slice(None)):
        @pl.loop(0, size // 8)
        def _(t):
            rows = pl.ds(pl.multiple_of(start + t * 8, 8), 8)
            acc[mask, rows, cols] += source[rows, cols]

    def take_pair(mask):
        pair_sum(mask).wait_recv()
        add_rows(mask, drecv.at[mask], 0, HID)
        for k in range(1, 4):
            for part in range(3):
                if reduce_unit(part, k)[1] == mask:
                    unit_copy(part, k).start()

    @pl.loop(0, 4)
    def _(q):
        other, half = 1 - q // 2, q % 2
        cols = pl.ds(pl.multiple_of(half * 512, 512), 512)
        acc[7 + 8 * other, :, cols] = jnp.dot(ut[...], abuf[(30 + other) % RING, :, cols], preferred_element_type=F32)
        for half in range(2):
            @pl.when(q == half)
            def _():
                pair_sum(7, half).start()

    for j in range(2):
        load_a(NDEV - 1 - j - RING, (31 - j) % RING).start()

    dw2_part = jnp.dot(gt[...], s2b[...], preferred_element_type=F32)
    d2src[...] = jnp.zeros_like(d2src)
    for j in range(6):
        for k in range(2):
            d2src[6 * k + j] = dw2_part[j * 8:(j + 1) * 8, k * 128:(k + 1) * 128]
    d2src[12] = jnp.full(TILE, loss_part, F32)
    d2src[13] = jnp.full(TILE, jnp.sum(weight), F32)
    keep_two = pltpu.make_async_copy(d2r2, d2out.at[me], xsem.at[0])
    d2r1[me] = d2src[me]
    small(1, d2src, d2r1, True)

    for half in range(2):
        pair_sum(7, half).wait_recv()
        add_rows(7, drecv.at[7], 0, HID, pl.ds(half * 512, 512))
        for part in range(3):
            unit_copy(part, 0, half).start()

    @pl.loop(1, 8)
    def _(p):
        for k in range(2):
            @pl.when(p >= 3)
            def _():
                wait_a((31 - 2 * p - k) % RING)
        for k in range(2):
            mask, other = step_order(NDEV - 1 - 2 * p - k)
            acc[mask + 8 * other] = jnp.dot(ut[...], abuf[(31 - 2 * p - k) % RING], preferred_element_type=F32)
        for k in range(2):
            @pl.when(p < 5)
            def _():
                load_a(NDEV - 1 - 2 * p - k - RING, (31 - 2 * p - k) % RING).start()

        for step in range(2, NDEV):
            step_mask, step_other = step_order(NDEV - 1 - step)

            @pl.when(p == step // 2)
            def _():
                if step_other:
                    pair_sum(step_mask).start()
                else:
                    take_pair(step_mask)

    def take_unit(part, k, send=None):
        axis, mask = reduce_unit(part, k)
        for c in unit_copies(part, k):
            c.wait_recv()
        add_rows(mask - (1 << axis), rbuf.at[k], *REDUCE_ROWS[part])
        if send is not None:
            unit_copy(part, send).start()

    for k in range(2):
        for part in range(3):
            take_unit(part, k, k + 4)
    for part in range(3):
        take_unit(part, 2)
    small_wait(1, d2r1)
    d2r2[...] = jnp.sum(d2r1[...], axis=0)
    for part in range(3):
        take_unit(part, 3)
    for part in range(3):
        take_unit(part, 4, 6)
    small(2, d2r2, d2out)
    keep_two.start()
    for k in (5, 6):
        for part in range(3):
            take_unit(part, k)

    grad_one = jnp.where(z1t[...] > 0.0, acc[0], 0.0).astype(BF16)
    d1src[...] = lax.dot_general(grad_one, s1b[...], NT, preferred_element_type=F32).reshape(NDEV, 16, FPAD)
    d1r1[me] = d1src[me]
    small(3, d1src, d1r1, True)
    drain_x()
    drain_h()
    remote(acc.at[pl.ds(0, 15)], acc.at[pl.ds(0, 15)], snd.at[2], pr.at[0], me).wait_send()
    small_wait(2, d2out)
    keep_two.wait()
    small_wait(3, d1r1)
    d1r2[...] = jnp.sum(d1r1[...], axis=0)
    small(4, d1r2, d1out)
    keep_one = pltpu.make_async_copy(d1r2, d1out.at[me], xsem.at[1])
    keep_one.start()
    keep_one.wait()
    small_wait(4, d1out)


def finish(d1_ref, d2_ref, loss_out, dw1_out, dw2_out):
    loss_out[...] = d2_ref[12, 0:1, 0:1] / d2_ref[13, 0:1, 0:1]
    dw1_out[...] = d1_ref[...].reshape(HID, FPAD).T[0:FIN, :]
    for k in range(2):
        dw2_out[:, pl.ds(k * 128, 128)] = d2_ref[pl.ds(6 * k, 6)].reshape(CPAD, 128)[0:NCLS]


def solution(mesh):
    def local_step(adj_rows, feat_rows, w_one, w_two, label_rows, mask_rows):
        vmem = pl.BlockSpec(memory_space=pltpu.VMEM)
        hbm = pl.BlockSpec(memory_space=pl.ANY)
        dma = pltpu.SemaphoreType.DMA
        parts = pl.pallas_call(
            kernel,
            out_shape=(jax.ShapeDtypeStruct((NDEV, 16, FPAD), F32), jax.ShapeDtypeStruct((NDEV, *TILE), F32)),
            in_specs=[hbm] * 6,
            out_specs=(hbm, hbm),
            scratch_shapes=[
                pltpu.VMEM((RING, BLK, BLK), BF16),
                pltpu.VMEM((FIN, BLK), BF16),
                pltpu.VMEM((FIN, HID), F32),
                pltpu.VMEM((NCLS, HID), F32),
                pltpu.VMEM((1, BLK), jnp.int32),
                pltpu.VMEM((1, BLK), jnp.int32),
                pltpu.VMEM((NDEV, FROWS, BLK), BF16),
                pltpu.VMEM((NDEV, BLK, HID), BF16),
                pltpu.VMEM((FPAD, BLK), F32),
                pltpu.VMEM((BLK, HID), F32),
                pltpu.VMEM((FPAD, BLK), BF16),
                pltpu.VMEM((BLK, HID), BF16),
                pltpu.VMEM((HID, BLK), F32),
                pltpu.VMEM((FPAD, HID), F32),
                pltpu.VMEM((HID, FPAD), BF16),
                pltpu.VMEM((CPAD, HID), BF16),
                pltpu.VMEM((HID, BLK), BF16),
                pltpu.VMEM((16, HID, BLK), F32),
                pltpu.VMEM((8, HID, BLK), F32),
                pltpu.VMEM((7, HID, BLK), F32),
                pltpu.VMEM((CPAD, BLK), BF16),
                pltpu.VMEM((NDEV, 1, 128), F32),
                *[pltpu.VMEM((NDEV, *TILE), F32)] * 2,
                pltpu.VMEM(TILE, F32),
                *[pltpu.VMEM((NDEV, 16, FPAD), F32)] * 2,
                pltpu.VMEM((16, FPAD), F32),
                *[dma((n,)) for n in (RING, 5, 42, 20, 24, 9, 5, 8)],
            ],
            compiler_params=pltpu.CompilerParams(collective_id=0, has_side_effects=True,
                                                 vmem_limit_bytes=67 * 1000 * 1000),
        )(adj_rows, feat_rows.T, w_one, w_two.T, label_rows.reshape(1, BLK), mask_rows.reshape(1, BLK))
        loss, dw_one, dw_two = pl.pallas_call(
            finish,
            out_shape=(jax.ShapeDtypeStruct((1, 1), F32), jax.ShapeDtypeStruct((FIN, HID), F32),
                       jax.ShapeDtypeStruct((NCLS, HID), F32)),
            in_specs=[vmem] * 2,
            out_specs=(vmem, vmem, vmem),
        )(*parts)
        return loss.reshape(1), dw_one, dw_two.T

    return jax.shard_map(local_step, mesh=mesh,
                         in_specs=(P(AXIS, None), P(AXIS, None), P(None, None), P(None, None), P(AXIS), P(AXIS)),
                         out_specs=(P(None), P(None, None), P(None, None)), check_vma=False)
```

```python
import functools

import jax
import jax.numpy as jnp
from jax import lax
from jax.experimental import pallas as pl
from jax.experimental.pallas import tpu as pltpu
from jax.sharding import PartitionSpec as P

MESH = pl.DeviceIdType.MESH
AXIS = 'nodes'
F32, BF16 = jnp.float32, jnp.bfloat16
NDEV = 16
BLK = 1024
FIN, FROWS, FPAD = 100, 104, 128
HID = 256
NCLS, CPAD = 47, 48
RING = 6
TILE = (8, 128)

ORDER = tuple((p, (p + 1) % 3, (p + 2) % 3) for p in range(3))
GATHER_ROWS = ((0, 352), (352, 336), (688, 336))
GATHER_COLS = ((0, 384), (384, 384), (768, 256))
REDUCE_ROWS = ((0, 88), (88, 88), (176, 80))

NT = (((1,), (1,)), ((), ()))
TN = (((0,), (0,)), ((), ()))


def gather_unit(axis, slot):
    first, second, third = axis, (axis + 2) % 3, (axis + 1) % 3
    if slot == 0:
        return first, 0
    if slot == 1:
        return second, 0
    if slot == 2:
        return third, 0
    if slot == 3:
        return second, 1 << ORDER[second][0]
    one, two = 1 << ORDER[third][0], 1 << ORDER[third][1]
    return third, {4: one, 5: two, 6: one | two}[slot]


def reduce_unit(part, k):
    b1, b2, b3 = ORDER[part]
    m1, m2, m3 = 1 << b1, 1 << b2, 1 << b3
    return ((b1, m1 | m2 | m3), (b1, m1 | m2), (b1, m1 | m3), (b1, m1), (b2, m2 | m3), (b2, m2), (b3, m3))[k]


def step_order(i):
    from2, from8, from10, from14 = ((i + 16 - n) // 16 for n in (2, 8, 10, 14))
    j = (i + 1) % 3
    one, xy, two = from2 - from8, from8 - from10, from10 - from14
    mask = one * ((j * j + j + 2) // 2) + xy * 3 + two * (5 + i % 2) + from14 * 7
    core = (1 - from2) * i + one * ((i + 1) // 3 - 1) + xy * (i - 8) + two * (i // 2 - 5) + from14 * (i - 14)
    return mask, core


def flip(bit, by):
    return bit + by - 2 * bit * by


def kernel(a_hbm, x_hbm, w1_hbm, w2_hbm, y_hbm, m_hbm, d1out, d2out,
           abuf, xin, w1_ref, w2_ref, y_ref, m_ref, xall, hall, s1acc, s2acc, s1b, s2b, z1t, w1p, w1t, w2t, ut,
           acc, drecv, rbuf, gt,
           cnt, d2src, d2r1, d2r2, d1src, d1r1, d1r2,
           asem, xsem, gr, dr, rr, er, pr, snd):
    me = lax.axis_index(AXIS)
    core, px, py, pz = me % 2, (me // 2) % 2, (me // 4) % 2, me // 8

    def dev(mask, other=0):
        fx, fy, fz, fc = mask % 2, (mask // 2) % 2, mask // 4, other
        return ((flip(pz, fz) * 2 + flip(py, fy)) * 2 + flip(px, fx)) * 2 + flip(core, fc)

    def block_of(i):
        mask, other = step_order(i)
        return dev(mask, other)

    def load_a(i, slot):
        start = pl.multiple_of(block_of(i) * BLK, BLK)
        return pltpu.make_async_copy(a_hbm.at[:, pl.ds(start, BLK)], abuf.at[slot], asem.at[slot])

    def wait_a(slot):
        pltpu.make_async_copy(a_hbm.at[:, pl.ds(0, BLK)], abuf.at[slot], asem.at[slot]).wait()

    def remote(src, dst, send, recv, to):
        return pltpu.make_async_remote_copy(src_ref=src, dst_ref=dst, send_sem=send, recv_sem=recv,
                                            device_id=(to,), device_id_type=MESH)

    def peer(d):
        return dev(d // 2, d % 2)

    far_first = sorted(range(1, NDEV), key=lambda d: -bin(d // 2).count('1'))

    barrier = pltpu.get_barrier_semaphore()
    for d in (8, 4, 2, 1):
        pl.semaphore_signal(barrier, inc=1, device_id=(peer(d),), device_id_type=MESH)
    loads = [pltpu.make_async_copy(src, dst, xsem.at[k]) for k, (src, dst) in enumerate((
        (x_hbm, xin), (m_hbm, m_ref), (w1_hbm, w1_ref), (w2_hbm, w2_ref), (y_hbm, y_ref)))]
    for load in loads:
        load.start()
    for i in range(RING):
        load_a(i, i).start()
    xall[me] = jnp.zeros((FROWS, BLK), BF16)
    loads[0].wait()
    xall[me, 0:FIN, :] = xin[...]
    loads[1].wait()
    cnt[me] = jnp.full((1, 128), jnp.sum(m_ref[...].astype(F32)), F32)
    pl.semaphore_wait(barrier, 4)

    def gather(buf, g):
        def piece(owner, part):
            return buf.at[owner, :, pl.ds(*GATHER_COLS[part])] if g == 0 else buf.at[owner, pl.ds(*GATHER_ROWS[part])]

        def copy(axis, slot):
            part, mask = gather_unit(axis, slot)
            ref = piece(dev(mask), part)
            n = g * 11 + (slot if slot < 4 else 4 if slot == 6 else 2 * axis + slot + 1)
            return remote(ref, ref, snd.at[g], gr.at[n], dev(1 << axis))

        def whole(sems, n):
            return remote(buf.at[me], buf.at[me], snd.at[g], sems.at[n], me)

        def give(*masks):
            for mask in masks:
                owner = dev(mask)
                for ref in [buf.at[owner]] if mask < 7 else [piece(owner, part) for part in range(3)]:
                    remote(ref, ref, snd.at[g], dr.at[g * 8 + mask], dev(0, 1)).start()

        def take(*masks):
            for mask in masks:
                whole(dr, g * 8 + mask).wait_recv()

        def begin():
            for slot in range(3):
                for axis in range(3):
                    copy(axis, slot).start()
            give(0)

        def forward(axis, slot, *onto):
            part, mask = gather_unit(axis, slot)
            for over, later in onto:
                assert gather_unit(over, later) == (part, mask | (1 << axis))
                copy(over, later).start()

        def arrive(*slots):
            for slot in slots:
                whole(gr, g * 11 + min(slot, 4)).wait_recv()

        def arrive_one(axis, slot):
            part, mask = gather_unit(axis, slot)
            ref = piece(dev(mask | (1 << axis)), part)
            remote(ref, ref, snd.at[g], gr.at[g * 11 + 2 * axis + slot + 1], me).wait_recv()

        def hooks(p):
            @pl.when(p == 0)
            def _():
                take(0)

            @pl.when(p == 1)
            def _():
                for slot in range(3):
                    arrive(slot)
                    for over in range(3):
                        if slot == 0:
                            forward((over + 2) % 3, 0, (over, 3))
                        if slot == 1:
                            forward((over + 2) % 3, 1, (over, 5))
                        if (slot == 0) == (over != 1) and slot < 2:
                            forward((over + 1) % 3, 0, (over, 4))
                give(1, 2, 4)

            @pl.when(p == 2)
            def _():
                take(1)

            @pl.when(p == 3)
            def _():
                take(2, 4)

            @pl.when(p == 4)
            def _():
                arrive(3)
                for over in range(3):
                    forward((over + 2) % 3, 3, (over, 6))
                arrive_one(1, 5)
                arrive_one(0, 4)
                give(3)
                take(3)

            @pl.when(p == 5)
            def _():
                arrive_one(2, 4)
                arrive_one(1, 4)
                arrive_one(0, 5)
                arrive_one(2, 5)
                give(5, 6)

            @pl.when(p == 6)
            def _():
                take(5, 6)

        def tail(i):
            @pl.when(i == 0)
            def _():
                arrive(6)
                give(7)

            @pl.when(i == 1)
            def _():
                take(7)

        def drain():
            every = buf.at[pl.ds(0, 15)]
            remote(every, every, snd.at[g], gr.at[g], me).wait_send()

        return begin, hooks, tail, drain

    def aggregate(buf, total, hooks, tail, g):
        def product(i):
            slot = (16 * g + i) % RING
            if g == 0:
                return lax.dot_general(buf[block_of(i)], abuf[slot], NT, preferred_element_type=F32)
            return jnp.dot(abuf[slot], buf[block_of(i)], preferred_element_type=F32)

        def refill(i):
            slot = (16 * g + i) % RING
            if g == 0:
                load_a((i + RING) % NDEV, slot).start()
            else:
                @pl.when(i < NDEV - RING)
                def _():
                    load_a(i + RING, slot).start()

        rows = pl.ds(0, FROWS if g == 0 else BLK)

        @pl.loop(0, 7)
        def _(p):
            hooks(p)
            wait_a((16 * g + 2 * p) % RING)
            wait_a((16 * g + 2 * p + 1) % RING)
            total[rows, :] += product(2 * p) + product(2 * p + 1)
            refill(2 * p)
            refill(2 * p + 1)

        @pl.loop(0, 2)
        def _(k):
            tail(k)
            wait_a((16 * g + 14 + k) % RING)
            total[rows, :] += product(14 + k)
            refill(14 + k)

    def small(x, src, dst, scatter=False):
        for d in far_first:
            remote(src.at[peer(d)] if scatter else src, dst.at[me], snd.at[3 + x], pr.at[x], peer(d)).start()

    def small_wait(x, dst):
        ref = dst.at[pl.ds(0, 15)]
        remote(ref, ref, snd.at[3 + x], pr.at[x], me).wait()

    begin_x, hooks_x, tail_x, drain_x = gather(xall, 0)
    begin_h, hooks_h, tail_h, drain_h = gather(hall, 1)

    begin_x()
    for load in loads[2:]:
        load.wait()
    w1p[...] = jnp.zeros_like(w1p)
    w1p[0:FIN, :] = w1_ref[...]
    w1t[...] = w1p[...].T.astype(BF16)
    w2t[...] = jnp.zeros_like(w2t)
    w2t[0:NCLS, :] = w2_ref[...].astype(BF16)
    s1acc[...] = jnp.zeros_like(s1acc)
    s2acc[...] = jnp.zeros_like(s2acc)
    aggregate(xall, s1acc, hooks_x, tail_x, 0)

    s1b[...] = s1acc[...].astype(BF16)
    pre_one = jnp.dot(s1acc[...].T.astype(BF16), w1p[...].astype(BF16), preferred_element_type=F32)
    hall[me] = jnp.maximum(pre_one, 0.0).astype(BF16)
    begin_h()
    small(0, cnt.at[me], cnt)
    z1t[...] = jnp.dot(w1t[...], s1b[...], preferred_element_type=F32)
    aggregate(hall, s2acc, hooks_h, tail_h, 1)

    small_wait(0, cnt)
    label_count = jnp.sum(cnt[...], axis=0)[0:1, 0:1]
    s2b[...] = s2acc[...].astype(BF16)
    logits = lax.dot_general(w2t[...], s2b[...], NT, preferred_element_type=F32)
    classes = lax.broadcasted_iota(jnp.int32, (CPAD, BLK), 0)
    logits = jnp.where(classes < NCLS, logits, -jnp.inf)
    shifted = logits - jnp.max(logits, axis=0, keepdims=True)
    log_prob = shifted - jnp.log(jnp.sum(jnp.exp(shifted), axis=0, keepdims=True))
    hit = classes == y_ref[...]
    weight = m_ref[...].astype(F32)
    picked = jnp.sum(jnp.where(hit, log_prob, 0.0), axis=0, keepdims=True)
    loss_part = -jnp.sum(weight * picked)
    grad = weight * (jnp.exp(log_prob) - jnp.where(hit, 1.0, 0.0)) / label_count
    gt[...] = grad.astype(BF16)
    ut[...] = lax.dot_general(w2t[...], gt[...], TN, preferred_element_type=F32).astype(BF16)

    def pair_sum(mask, half=None):
        if half is None:
            return remote(acc.at[8 + mask], drecv.at[mask], snd.at[2], er.at[mask], dev(0, 1))
        cols = pl.ds(half * 512, 512)
        return remote(acc.at[8 + mask, :, cols], drecv.at[mask, :, cols], snd.at[2], er.at[mask + half],
                      dev(0, 1))

    def unit_copy(part, k, half=None):
        axis, mask = reduce_unit(part, k)
        rows = pl.ds(*REDUCE_ROWS[part])
        if half is None:
            return remote(acc.at[mask, rows], rbuf.at[k, rows], snd.at[2], rr.at[k], dev(1 << axis))
        cols = pl.ds(half * 512, 512)
        return remote(acc.at[mask, rows, cols], rbuf.at[k, rows, cols], snd.at[2], rr.at[k], dev(1 << axis))

    def add_rows(mask, source, start, size, cols=slice(None)):
        @pl.loop(0, size // 8)
        def _(t):
            rows = pl.ds(pl.multiple_of(start + t * 8, 8), 8)
            acc[mask, rows, cols] += source[rows, cols]

    def take_pair(mask):
        pair_sum(mask).wait_recv()
        add_rows(mask, drecv.at[mask], 0, HID)
        for k in range(1, 4):
            for part in range(3):
                if reduce_unit(part, k)[1] == mask:
                    unit_copy(part, k).start()

    @pl.loop(0, 4)
    def _(q):
        other, half = 1 - q // 2, q % 2
        cols = pl.ds(pl.multiple_of(half * 512, 512), 512)
        acc[7 + 8 * other, :, cols] = jnp.dot(ut[...], abuf[(30 + other) % RING, :, cols], preferred_element_type=F32)
        for half in range(2):
            @pl.when(q == half)
            def _():
                pair_sum(7, half).start()

    for j in range(2):
        load_a(NDEV - 1 - j - RING, (31 - j) % RING).start()

    dw2_part = jnp.dot(gt[...], s2b[...], preferred_element_type=F32)
    d2src[...] = jnp.zeros_like(d2src)
    for j in range(6):
        for k in range(2):
            d2src[6 * k + j] = dw2_part[j * 8:(j + 1) * 8, k * 128:(k + 1) * 128]
    d2src[12] = jnp.full(TILE, loss_part, F32)
    d2src[13] = jnp.full(TILE, jnp.sum(weight), F32)
    keep_two = pltpu.make_async_copy(d2r2, d2out.at[me], xsem.at[0])
    d2r1[me] = d2src[me]
    small(1, d2src, d2r1, True)

    for half in range(2):
        pair_sum(7, half).wait_recv()
        add_rows(7, drecv.at[7], 0, HID, pl.ds(half * 512, 512))
        for part in range(3):
            unit_copy(part, 0, half).start()

    @pl.loop(1, 8)
    def _(p):
        for k in range(2):
            @pl.when(p >= 3)
            def _():
                wait_a((31 - 2 * p - k) % RING)
        for k in range(2):
            mask, other = step_order(NDEV - 1 - 2 * p - k)
            acc[mask + 8 * other] = jnp.dot(ut[...], abuf[(31 - 2 * p - k) % RING], preferred_element_type=F32)
        for k in range(2):
            @pl.when(p < 5)
            def _():
                load_a(NDEV - 1 - 2 * p - k - RING, (31 - 2 * p - k) % RING).start()

        for step in range(2, NDEV):
            step_mask, step_other = step_order(NDEV - 1 - step)

            @pl.when(p == step // 2)
            def _():
                if step_other:
                    pair_sum(step_mask).start()
                else:
                    take_pair(step_mask)

    def units_wait(k):
        remote(rbuf.at[k], rbuf.at[k], snd.at[2], rr.at[k], me).wait_recv()

    def take_units(k, send=None):
        units_wait(k)
        for part in range(3):
            axis, mask = reduce_unit(part, k)
            add_rows(mask - (1 << axis), rbuf.at[k], *REDUCE_ROWS[part])
            if send is not None:
                unit_copy(part, send).start()

    take_units(0, 4)
    take_units(1, 5)
    take_units(2)
    small_wait(1, d2r1)
    d2r2[...] = jnp.sum(d2r1[...], axis=0)
    take_units(3)
    take_units(4, 6)
    small(2, d2r2, d2out)
    keep_two.start()
    take_units(5)
    units_wait(6)
    grad_one = jnp.where(z1t[...] > 0.0, acc[0] + rbuf[6], 0.0).astype(BF16)
    d1src[...] = lax.dot_general(grad_one, s1b[...], NT, preferred_element_type=F32).reshape(NDEV, 16, FPAD)
    d1r1[me] = d1src[me]
    small(3, d1src, d1r1, True)
    drain_x()
    drain_h()
    remote(acc.at[pl.ds(0, 15)], acc.at[pl.ds(0, 15)], snd.at[2], pr.at[0], me).wait_send()
    small_wait(2, d2out)
    keep_two.wait()
    small_wait(3, d1r1)
    d1r2[...] = jnp.sum(d1r1[...], axis=0)
    small(4, d1r2, d1out)
    keep_one = pltpu.make_async_copy(d1r2, d1out.at[me], xsem.at[1])
    keep_one.start()
    keep_one.wait()
    small_wait(4, d1out)


def finish(d1_ref, d2_ref, loss_out, dw1_out, dw2_out):
    loss_out[...] = d2_ref[12, 0:1, 0:1] / d2_ref[13, 0:1, 0:1]
    dw1_out[...] = d1_ref[...].reshape(HID, FPAD).T[0:FIN, :]
    for k in range(2):
        dw2_out[:, pl.ds(k * 128, 128)] = d2_ref[pl.ds(6 * k, 6)].reshape(CPAD, 128)[0:NCLS]


def solution(mesh):
    def local_step(adj_rows, feat_rows, w_one, w_two, label_rows, mask_rows):
        vmem = pl.BlockSpec(memory_space=pltpu.VMEM)
        hbm = pl.BlockSpec(memory_space=pl.ANY)
        dma = pltpu.SemaphoreType.DMA
        parts = pl.pallas_call(
            kernel,
            out_shape=(jax.ShapeDtypeStruct((NDEV, 16, FPAD), F32), jax.ShapeDtypeStruct((NDEV, *TILE), F32)),
            in_specs=[hbm] * 6,
            out_specs=(hbm, hbm),
            scratch_shapes=[
                pltpu.VMEM((RING, BLK, BLK), BF16),
                pltpu.VMEM((FIN, BLK), BF16),
                pltpu.VMEM((FIN, HID), F32),
                pltpu.VMEM((NCLS, HID), F32),
                pltpu.VMEM((1, BLK), jnp.int32),
                pltpu.VMEM((1, BLK), jnp.int32),
                pltpu.VMEM((NDEV, FROWS, BLK), BF16),
                pltpu.VMEM((NDEV, BLK, HID), BF16),
                pltpu.VMEM((FPAD, BLK), F32),
                pltpu.VMEM((BLK, HID), F32),
                pltpu.VMEM((FPAD, BLK), BF16),
                pltpu.VMEM((BLK, HID), BF16),
                pltpu.VMEM((HID, BLK), F32),
                pltpu.VMEM((FPAD, HID), F32),
                pltpu.VMEM((HID, FPAD), BF16),
                pltpu.VMEM((CPAD, HID), BF16),
                pltpu.VMEM((HID, BLK), BF16),
                pltpu.VMEM((16, HID, BLK), F32),
                pltpu.VMEM((8, HID, BLK), F32),
                pltpu.VMEM((7, HID, BLK), F32),
                pltpu.VMEM((CPAD, BLK), BF16),
                pltpu.VMEM((NDEV, 1, 128), F32),
                *[pltpu.VMEM((NDEV, *TILE), F32)] * 2,
                pltpu.VMEM(TILE, F32),
                *[pltpu.VMEM((NDEV, 16, FPAD), F32)] * 2,
                pltpu.VMEM((16, FPAD), F32),
                *[dma((n,)) for n in (RING, 5, 22, 16, 7, 9, 5, 8)],
            ],
            compiler_params=pltpu.CompilerParams(collective_id=0, has_side_effects=True,
                                                 vmem_limit_bytes=67 * 1000 * 1000),
        )(adj_rows, feat_rows.T, w_one, w_two.T, label_rows.reshape(1, BLK), mask_rows.reshape(1, BLK))
        loss, dw_one, dw_two = pl.pallas_call(
            finish,
            out_shape=(jax.ShapeDtypeStruct((1, 1), F32), jax.ShapeDtypeStruct((FIN, HID), F32),
                       jax.ShapeDtypeStruct((NCLS, HID), F32)),
            in_specs=[vmem] * 2,
            out_specs=(vmem, vmem, vmem),
        )(*parts)
        return loss.reshape(1), dw_one, dw_two.T

    return jax.shard_map(local_step, mesh=mesh,
                         in_specs=(P(AXIS, None), P(AXIS, None), P(None, None), P(None, None), P(AXIS), P(AXIS)),
                         out_specs=(P(None), P(None, None), P(None, None)), check_vma=False)
```

```python
import functools

import jax
import jax.numpy as jnp
from jax import lax
from jax.experimental import pallas as pl
from jax.experimental.pallas import tpu as pltpu
from jax.sharding import PartitionSpec as P

MESH = pl.DeviceIdType.MESH
AXIS = 'nodes'
F32, BF16 = jnp.float32, jnp.bfloat16
NDEV = 16
BLK = 1024
FIN, FROWS, FPAD = 100, 104, 128
HID = 256
NCLS, CPAD = 47, 48
RING = 6
TILE = (8, 128)

AXES, BOTH = range(3), range(2)
BIT = (1, 2, 4)
SOURCE = (0, 0, 0, 1, 1, 2, 4)
ORDER = tuple((p, (p + 1) % 3, (p + 2) % 3) for p in AXES)
GATHER_ROWS = ((0, 352), (352, 336), (688, 336))
GATHER_COLS = ((0, 384), (384, 384), (768, 256))
REDUCE_ROWS = ((0, 88), (88, 88), (176, 80))

NT = (((1,), (1,)), ((), ()))
TN = (((0,), (0,)), ((), ()))


def gather_unit(axis, slot):
    first, second, third = axis, (axis + 2) % 3, (axis + 1) % 3
    if slot == 0:
        return first, 0
    if slot == 1:
        return second, 0
    if slot == 2:
        return third, 0
    if slot == 3:
        return second, 1 << ORDER[second][0]
    one, two = 1 << ORDER[third][0], 1 << ORDER[third][1]
    return third, {4: one, 5: two, 6: one | two}[slot]


def reduce_unit(part, k):
    b1, b2, b3 = ORDER[part]
    m1, m2, m3 = BIT[b1], BIT[b2], BIT[b3]
    return ((b1, m1 | m2 | m3), (b1, m1 | m2), (b1, m1 | m3), (b1, m1), (b2, m2 | m3), (b2, m2), (b3, m3))[k]


def step_order(i):
    from2, from8, from10, from14 = ((i + 16 - n) // 16 for n in (2, 8, 10, 14))
    j = (i + 1) % 3
    one, xy, two = from2 - from8, from8 - from10, from10 - from14
    mask = one * ((j * j + j + 2) // 2) + xy * 3 + two * (5 + i % 2) + from14 * 7
    core = (1 - from2) * i + one * ((i + 1) // 3 - 1) + xy * (i - 8) + two * (i // 2 - 5) + from14 * (i - 14)
    return mask, core


def mixed_order(i):
    first, last = 1 - (i + 15) // 16, i // 15
    core = (1 - first) * (1 - last) * ((i + 1) % 2) + last
    return (i + 1) // 2 - core * (1 - last) - last, core


def mixed_mask(part, v):
    code = v + (v + 5) // 8 - 2 * ((v + 4) // 8) + (v + 3) // 8
    m1, m2, m3 = (BIT[axis] for axis in ORDER[part])
    return (code % 2) * m1 + ((code // 2) % 2) * m2 + (code // 4) * m3


def flip(bit, by):
    return bit + by - 2 * bit * by


def kernel(a_hbm, x_hbm, w1_hbm, w2_hbm, y_hbm, m_hbm, d1out, d2out,
           abuf, xin, w1_ref, w2_ref, y_ref, m_ref, xall, hall, s1acc, s2acc, s1b, s2b, z1t, w1p, w1t, w2t, ut,
           acc, drecv, rbuf, gt,
           cnt, d2src, d2r1, d2r2, d1src, d1r1, d1r2,
           asem, xsem, gr, dr, rr, er, pr, snd):
    me = lax.axis_index(AXIS)
    core, px, py, pz = me % 2, (me // 2) % 2, (me // 4) % 2, me // 8

    def dev(mask, other=0):
        fx, fy, fz, fc = mask % 2, (mask // 2) % 2, mask // 4, other
        return ((flip(pz, fz) * 2 + flip(py, fy)) * 2 + flip(px, fx)) * 2 + flip(core, fc)

    def block_of(i):
        mask, other = step_order(i)
        return dev(mask, other)

    def load_a(i, slot):
        start = pl.multiple_of(block_of(i) * BLK, BLK)
        return pltpu.make_async_copy(a_hbm.at[:, pl.ds(start, BLK)], abuf.at[slot], asem.at[slot])

    def load_mixed(i, slot):
        v, other = mixed_order(i)
        for part, (start, size) in enumerate(GATHER_COLS):
            begin = pl.multiple_of(dev(mixed_mask(part, v), other) * BLK + start, 128)
            pltpu.make_async_copy(a_hbm.at[:, pl.ds(begin, size)], abuf.at[slot, :, pl.ds(start, size)],
                                  asem.at[slot]).start()

    def wait_a(slot):
        pltpu.make_async_copy(a_hbm.at[:, pl.ds(0, BLK)], abuf.at[slot], asem.at[slot]).wait()

    twin = dev(0, 1)

    def remote(src, dst, send, recv, to):
        return pltpu.make_async_remote_copy(src_ref=src, dst_ref=dst, send_sem=send, recv_sem=recv,
                                            device_id=(to,), device_id_type=MESH)

    def peer(d):
        return dev(d // 2, d % 2)

    far_first = sorted(range(1, NDEV), key=lambda d: -bin(d // 2).count('1'))

    barrier = pltpu.get_barrier_semaphore()
    for d in (8, 4, 2, 1):
        pl.semaphore_signal(barrier, inc=1, device_id=(peer(d),), device_id_type=MESH)
    loads = [pltpu.make_async_copy(src, dst, xsem.at[k]) for k, (src, dst) in enumerate((
        (x_hbm, xin), (m_hbm, m_ref), (w1_hbm, w1_ref), (w2_hbm, w2_ref), (y_hbm, y_ref)))]
    for load in loads:
        load.start()
    for i in range(RING):
        load_mixed(i, i)
    xall[0] = jnp.zeros((FROWS, BLK), BF16)
    loads[0].wait()
    xall[0, 0:FIN, :] = xin[...]
    loads[1].wait()
    cnt[me] = jnp.full((1, 128), jnp.sum(m_ref[...].astype(F32)), F32)
    pl.semaphore_wait(barrier, 4)

    def mixed_copy(axis, slot):
        cols = pl.ds(*GATHER_COLS[gather_unit(axis, slot)[0]])
        return remote(xall.at[SOURCE[slot], :, cols], xall.at[slot + 1, :, cols], snd.at[0], gr.at[slot], dev(BIT[axis]))

    def mixed_start(*slots):
        for slot in slots:
            for axis in AXES:
                mixed_copy(axis, slot).start()

    def mixed_give(v):
        remote(xall.at[v], xall.at[8 + v], snd.at[0], dr.at[v], twin).start()

    def mixed_take(sems, n):
        remote(xall.at[0], xall.at[0], snd.at[0], sems.at[n], me).wait_recv()

    def mixed_product(i):
        v, other = mixed_order(i)
        return lax.dot_general(xall[8 * other + v], abuf[i % RING], NT, preferred_element_type=F32)

    def mixed_refill(i):
        @pl.when(i < NDEV - RING)
        def _():
            load_mixed(i + RING, i % RING)

        @pl.when(i >= NDEV - RING)
        def _():
            load_a(i + RING - NDEV, i % RING).start()

    def aggregate_features():
        wait_a(0)
        s1acc[0:FROWS, :] += mixed_product(0)
        mixed_refill(0)

        @pl.loop(0, 7)
        def _(slot):
            for k in range(7):
                @pl.when(slot == k)
                def _():
                    mixed_take(gr, k)
                    mixed_start(*(later for later in range(3, 7) if SOURCE[later] == k + 1))
                    mixed_give(k + 1)
            mixed_take(dr, slot)
            i = 2 * slot + 1
            wait_a(i % RING)
            wait_a((i + 1) % RING)
            s1acc[0:FROWS, :] += mixed_product(i) + mixed_product(i + 1)
            mixed_refill(i)
            mixed_refill(i + 1)

        mixed_take(dr, 7)
        wait_a((NDEV - 1) % RING)
        s1acc[0:FROWS, :] += mixed_product(NDEV - 1)
        mixed_refill(NDEV - 1)

    def gather(buf, g):
        def piece(owner, part):
            return buf.at[owner, pl.ds(*GATHER_ROWS[part])]

        def copy(axis, slot):
            part, mask = gather_unit(axis, slot)
            ref = piece(dev(mask), part)
            n = 7 + (slot if slot < 4 else 4 if slot == 6 else 2 * axis + slot + 1)
            return remote(ref, ref, snd.at[g], gr.at[n], dev(BIT[axis]))

        def whole(sems, n):
            return remote(buf.at[me], buf.at[me], snd.at[g], sems.at[n], me)

        def give(*masks):
            for mask in masks:
                owner = dev(mask)
                for ref in [buf.at[owner]] if mask < 7 else [piece(owner, part) for part in AXES]:
                    remote(ref, ref, snd.at[g], dr.at[8 + mask], twin).start()

        def take(*masks):
            for mask in masks:
                whole(dr, 8 + mask).wait_recv()

        def begin():
            for slot in AXES:
                for axis in AXES:
                    copy(axis, slot).start()
            give(0)

        def forward(axis, slot, *onto):
            part, mask = gather_unit(axis, slot)
            for over, later in onto:
                assert gather_unit(over, later) == (part, mask | BIT[axis])
                copy(over, later).start()

        def arrive(*slots):
            for slot in slots:
                whole(gr, 7 + min(slot, 4)).wait_recv()

        def arrive_one(axis, slot):
            part, mask = gather_unit(axis, slot)
            ref = piece(dev(mask | BIT[axis]), part)
            remote(ref, ref, snd.at[g], gr.at[8 + 2 * axis + slot], me).wait_recv()

        def hooks(p):
            @pl.when(p == 0)
            def _():
                take(0)

            @pl.when(p == 1)
            def _():
                for slot in AXES:
                    arrive(slot)
                    for over in AXES:
                        if slot == 0:
                            forward((over + 2) % 3, 0, (over, 3))
                        if slot == 1:
                            forward((over + 2) % 3, 1, (over, 5))
                        if (slot == 0) == (over != 1) and slot < 2:
                            forward((over + 1) % 3, 0, (over, 4))
                give(1, 2, 4)

            @pl.when(p == 2)
            def _():
                take(1)

            @pl.when(p == 3)
            def _():
                take(2, 4)

            @pl.when(p == 4)
            def _():
                arrive(3)
                for over in AXES:
                    forward((over + 2) % 3, 3, (over, 6))
                arrive_one(1, 5)
                arrive_one(0, 4)
                give(3)
                take(3)

            @pl.when(p == 5)
            def _():
                arrive_one(2, 4)
                arrive_one(1, 4)
                arrive_one(0, 5)
                arrive_one(2, 5)
                give(5, 6)

            @pl.when(p == 6)
            def _():
                take(5, 6)

        def tail(i):
            @pl.when(i == 0)
            def _():
                arrive(6)
                give(7)

            @pl.when(i == 1)
            def _():
                take(7)

        return begin, hooks, tail

    def drain(buf, n):
        every = buf.at[pl.ds(0, 15)]
        remote(every, every, snd.at[n], gr.at[n], me).wait_send()

    def aggregate(buf, total, hooks, tail):
        def product(i):
            return jnp.dot(abuf[(NDEV + i) % RING], buf[block_of(i)], preferred_element_type=F32)

        def refill(i):
            @pl.when(i < NDEV - RING)
            def _():
                load_a(i + RING, (NDEV + i) % RING).start()

        @pl.loop(0, 7)
        def _(p):
            hooks(p)
            for k in BOTH:
                wait_a((NDEV + 2 * p + k) % RING)
            total[...] += product(2 * p) + product(2 * p + 1)
            for k in BOTH:
                refill(2 * p + k)

        @pl.loop(0, 2)
        def _(k):
            tail(k)
            wait_a((NDEV + 14 + k) % RING)
            total[...] += product(14 + k)

    def small(x, src, dst, scatter=False):
        for d in far_first:
            remote(src.at[peer(d)] if scatter else src, dst.at[me], snd.at[3 + x], pr.at[x], peer(d)).start()

    def small_wait(x, dst):
        ref = dst.at[pl.ds(0, 15)]
        remote(ref, ref, snd.at[3 + x], pr.at[x], me).wait()

    begin_h, hooks_h, tail_h = gather(hall, 1)

    mixed_start(0, 1, 2)
    mixed_give(0)
    for load in loads[2:]:
        load.wait()
    w1p[...] = jnp.zeros_like(w1p)
    w1p[0:FIN, :] = w1_ref[...]
    w1t[...] = w1p[...].T.astype(BF16)
    w2t[...] = jnp.zeros_like(w2t)
    w2t[0:NCLS, :] = w2_ref[...].astype(BF16)
    s1acc[...] = jnp.zeros_like(s1acc)
    s2acc[...] = jnp.zeros_like(s2acc)
    aggregate_features()

    s1b[...] = s1acc[...].astype(BF16)
    pre_one = jnp.dot(s1acc[...].T.astype(BF16), w1p[...].astype(BF16), preferred_element_type=F32)
    hall[me] = jnp.maximum(pre_one, 0.0).astype(BF16)
    begin_h()
    small(0, cnt.at[me], cnt)
    z1t[...] = jnp.dot(w1t[...], s1b[...], preferred_element_type=F32)
    aggregate(hall, s2acc, hooks_h, tail_h)

    small_wait(0, cnt)
    label_count = jnp.sum(cnt[...], axis=0)[0:1, 0:1]
    s2b[...] = s2acc[...].astype(BF16)
    logits = lax.dot_general(w2t[...], s2b[...], NT, preferred_element_type=F32)
    classes = lax.broadcasted_iota(jnp.int32, (CPAD, BLK), 0)
    logits = jnp.where(classes < NCLS, logits, -jnp.inf)
    shifted = logits - jnp.max(logits, axis=0, keepdims=True)
    log_prob = shifted - jnp.log(jnp.sum(jnp.exp(shifted), axis=0, keepdims=True))
    hit = classes == y_ref[...]
    weight = m_ref[...].astype(F32)
    picked = jnp.sum(jnp.where(hit, log_prob, 0.0), axis=0, keepdims=True)
    loss_part = -jnp.sum(weight * picked)
    grad = weight * (jnp.exp(log_prob) - jnp.where(hit, 1.0, 0.0)) / label_count
    gt[...] = grad.astype(BF16)
    ut[...] = lax.dot_general(w2t[...], gt[...], TN, preferred_element_type=F32).astype(BF16)

    def pair_sum(mask, half=None):
        if half is None:
            return remote(acc.at[8 + mask], drecv.at[mask], snd.at[2], er.at[mask], twin)
        cols = pl.ds(half * 512, 512)
        return remote(acc.at[8 + mask, :, cols], drecv.at[mask, :, cols], snd.at[2], er.at[mask + half],
                      twin)

    def unit_copy(part, k, half=None):
        axis, mask = reduce_unit(part, k)
        rows = pl.ds(*REDUCE_ROWS[part])
        if half is None:
            return remote(acc.at[mask, rows], rbuf.at[k, rows], snd.at[2], rr.at[k], dev(BIT[axis]))
        cols = pl.ds(half * 512, 512)
        return remote(acc.at[mask, rows, cols], rbuf.at[k, rows, cols], snd.at[2], rr.at[k], dev(BIT[axis]))

    def add_rows(mask, source, start, size, cols=slice(None)):
        @pl.loop(0, size // 8)
        def _(t):
            rows = pl.ds(pl.multiple_of(start + t * 8, 8), 8)
            acc[mask, rows, cols] += source[rows, cols]

    def take_pair(mask):
        pair_sum(mask).wait_recv()
        add_rows(mask, drecv.at[mask], 0, HID)
        for k in range(1, 4):
            for part in AXES:
                if reduce_unit(part, k)[1] == mask:
                    unit_copy(part, k).start()

    @pl.loop(0, 4)
    def _(q):
        other, half = 1 - q // 2, q % 2
        cols = pl.ds(pl.multiple_of(half * 512, 512), 512)
        acc[7 + 8 * other, :, cols] = jnp.dot(ut[...], abuf[(30 + other) % RING, :, cols], preferred_element_type=F32)
        for half in BOTH:
            @pl.when(q == half)
            def _():
                pair_sum(7, half).start()

    for j in BOTH:
        load_a(NDEV - 1 - j - RING, (31 - j) % RING).start()

    dw2_part = jnp.dot(gt[...], s2b[...], preferred_element_type=F32)
    d2src[...] = jnp.zeros_like(d2src)
    for j in range(6):
        for k in BOTH:
            d2src[6 * k + j] = dw2_part[j * 8:(j + 1) * 8, k * 128:(k + 1) * 128]
    d2src[12] = jnp.full(TILE, loss_part, F32)
    d2src[13] = jnp.full(TILE, jnp.sum(weight), F32)
    keep_two = pltpu.make_async_copy(d2r2, d2out.at[me], xsem.at[0])
    d2r1[me] = d2src[me]
    small(1, d2src, d2r1, True)

    for half in BOTH:
        pair_sum(7, half).wait_recv()
        add_rows(7, drecv.at[7], 0, HID, pl.ds(half * 512, 512))
        for part in AXES:
            unit_copy(part, 0, half).start()

    @pl.loop(1, 8)
    def _(p):
        for k in BOTH:
            @pl.when(p >= 3)
            def _():
                wait_a((31 - 2 * p - k) % RING)
        for k in BOTH:
            mask, other = step_order(NDEV - 1 - 2 * p - k)
            acc[mask + 8 * other] = jnp.dot(ut[...], abuf[(31 - 2 * p - k) % RING], preferred_element_type=F32)
        for k in BOTH:
            @pl.when(p < 5)
            def _():
                load_a(NDEV - 1 - 2 * p - k - RING, (31 - 2 * p - k) % RING).start()

        for step in range(2, NDEV):
            step_mask, step_other = step_order(NDEV - 1 - step)

            @pl.when(p == step // 2)
            def _():
                if step_other:
                    pair_sum(step_mask).start()
                else:
                    take_pair(step_mask)

    def units_wait(k):
        remote(rbuf.at[k], rbuf.at[k], snd.at[2], rr.at[k], me).wait_recv()

    def take_units(k, send=None):
        units_wait(k)
        for part in AXES:
            axis, mask = reduce_unit(part, k)
            add_rows(mask - BIT[axis], rbuf.at[k], *REDUCE_ROWS[part])
            if send is not None:
                unit_copy(part, send).start()

    take_units(0, 4)
    take_units(1, 5)
    take_units(2)
    small_wait(1, d2r1)
    d2r2[...] = jnp.sum(d2r1[...], axis=0)
    take_units(3)
    take_units(4, 6)
    small(2, d2r2, d2out)
    keep_two.start()
    take_units(5)
    units_wait(6)
    grad_one = jnp.where(z1t[...] > 0.0, acc[0] + rbuf[6], 0.0).astype(BF16)
    d1src[...] = lax.dot_general(grad_one, s1b[...], NT, preferred_element_type=F32).reshape(NDEV, 16, FPAD)
    d1r1[me] = d1src[me]
    small(3, d1src, d1r1, True)
    for n, buf in enumerate((xall, hall, acc)):
        drain(buf, n)
    small_wait(2, d2out)
    keep_two.wait()
    small_wait(3, d1r1)
    d1r2[...] = jnp.sum(d1r1[...], axis=0)
    small(4, d1r2, d1out)
    keep_one = pltpu.make_async_copy(d1r2, d1out.at[me], xsem.at[1])
    keep_one.start()
    keep_one.wait()
    small_wait(4, d1out)


def finish(d1_ref, d2_ref, loss_out, dw1_out, dw2_out):
    loss_out[...] = d2_ref[12, 0:1, 0:1] / d2_ref[13, 0:1, 0:1]
    dw1_out[...] = d1_ref[...].reshape(HID, FPAD).T[0:FIN, :]
    for k in BOTH:
        dw2_out[:, pl.ds(k * 128, 128)] = d2_ref[pl.ds(6 * k, 6)].reshape(CPAD, 128)[0:NCLS]


def solution(mesh):
    def local_step(adj_rows, feat_rows, w_one, w_two, label_rows, mask_rows):
        vmem = pl.BlockSpec(memory_space=pltpu.VMEM)
        hbm = pl.BlockSpec(memory_space=pl.ANY)
        dma = pltpu.SemaphoreType.DMA
        parts = pl.pallas_call(
            kernel,
            out_shape=(jax.ShapeDtypeStruct((NDEV, 16, FPAD), F32), jax.ShapeDtypeStruct((NDEV, *TILE), F32)),
            in_specs=[hbm] * 6,
            out_specs=(hbm, hbm),
            scratch_shapes=[
                pltpu.VMEM((RING, BLK, BLK), BF16),
                pltpu.VMEM((FIN, BLK), BF16),
                pltpu.VMEM((FIN, HID), F32),
                pltpu.VMEM((NCLS, HID), F32),
                pltpu.VMEM((1, BLK), jnp.int32),
                pltpu.VMEM((1, BLK), jnp.int32),
                pltpu.VMEM((NDEV, FROWS, BLK), BF16),
                pltpu.VMEM((NDEV, BLK, HID), BF16),
                pltpu.VMEM((FPAD, BLK), F32),
                pltpu.VMEM((BLK, HID), F32),
                pltpu.VMEM((FPAD, BLK), BF16),
                pltpu.VMEM((BLK, HID), BF16),
                pltpu.VMEM((HID, BLK), F32),
                pltpu.VMEM((FPAD, HID), F32),
                pltpu.VMEM((HID, FPAD), BF16),
                pltpu.VMEM((CPAD, HID), BF16),
                pltpu.VMEM((HID, BLK), BF16),
                pltpu.VMEM((16, HID, BLK), F32),
                pltpu.VMEM((8, HID, BLK), F32),
                pltpu.VMEM((7, HID, BLK), F32),
                pltpu.VMEM((CPAD, BLK), BF16),
                pltpu.VMEM((NDEV, 1, 128), F32),
                *[pltpu.VMEM((NDEV, *TILE), F32)] * 2,
                pltpu.VMEM(TILE, F32),
                *[pltpu.VMEM((NDEV, 16, FPAD), F32)] * 2,
                pltpu.VMEM((16, FPAD), F32),
                *[dma((n,)) for n in (RING, 5, 18, 16, 7, 9, 5, 8)],
            ],
            compiler_params=pltpu.CompilerParams(collective_id=0, has_side_effects=True,
                                                 vmem_limit_bytes=67 * 1000 * 1000),
        )(adj_rows, feat_rows.T, w_one, w_two.T, label_rows.reshape(1, BLK), mask_rows.reshape(1, BLK))
        loss, dw_one, dw_two = pl.pallas_call(
            finish,
            out_shape=(jax.ShapeDtypeStruct((1, 1), F32), jax.ShapeDtypeStruct((FIN, HID), F32),
                       jax.ShapeDtypeStruct((NCLS, HID), F32)),
            in_specs=[vmem] * 2,
            out_specs=(vmem, vmem, vmem),
        )(*parts)
        return loss.reshape(1), dw_one, dw_two.T

    return jax.shard_map(local_step, mesh=mesh,
                         in_specs=(P(AXIS, None), P(AXIS, None), P(None, None), P(None, None), P(AXIS), P(AXIS)),
                         out_specs=(P(None), P(None, None), P(None, None)), check_vma=False)
```

```python
import functools

import jax
import jax.numpy as jnp
from jax import lax
from jax.experimental import pallas as pl
from jax.experimental.pallas import tpu as pltpu
from jax.sharding import PartitionSpec as P

MESH = pl.DeviceIdType.MESH
AXIS = 'nodes'
F32, BF16 = jnp.float32, jnp.bfloat16
NDEV = 16
BLK = 1024
FIN, FROWS, FPAD = 100, 104, 128
HID = 256
NCLS, CPAD = 47, 48
RING = 6
TILE = (8, 128)

AXES, BOTH = range(3), range(2)
BIT = (1, 2, 4)
ORDER = tuple((p, (p + 1) % 3, (p + 2) % 3) for p in AXES)
GATHER_ROWS = ((0, 352), (352, 336), (688, 336))
MIXED_ORDER = (*ORDER, (0, 2, 1))
MIXED_COLS = ((0, 256), (256, 384), (640, 256), (896, 128))
REDUCE_ROWS = ((0, 88), (88, 88), (176, 80))

NT = (((1,), (1,)), ((), ()))
TN = (((0,), (0,)), ((), ()))


CODE = (0, 1, 2, 4, 3, 5, 6, 7)
VIA = [code.bit_length() - 1 for code in CODE[1:]]
SOURCE = [CODE.index(code - (1 << via)) for code, via in zip(CODE[1:], VIA)]


def gather_unit(axis, slot):
    part = next(p for p in AXES if ORDER[p][VIA[slot]] == axis)
    return part, sum(BIT[ORDER[part][j]] for j in AXES if CODE[SOURCE[slot]] >> j & 1)


def reduce_unit(part, k):
    b1, b2, b3 = ORDER[part]
    m1, m2, m3 = BIT[b1], BIT[b2], BIT[b3]
    return ((b1, m1 | m2 | m3), (b1, m1 | m2), (b1, m1 | m3), (b1, m1), (b2, m2 | m3), (b2, m2), (b3, m3))[k]


def step_order(i):
    from2, from8, from10, from14 = ((i + 16 - n) // 16 for n in (2, 8, 10, 14))
    j = (i + 1) % 3
    one, xy, two = from2 - from8, from8 - from10, from10 - from14
    mask = one * ((j * j + j + 2) // 2) + xy * 3 + two * (5 + i % 2) + from14 * 7
    core = (1 - from2) * i + one * ((i + 1) // 3 - 1) + xy * (i - 8) + two * (i // 2 - 5) + from14 * (i - 14)
    return mask, core


def mixed_order(i):
    first, last = 1 - (i + 15) // 16, i // 15
    core = (1 - first) * (1 - last) * ((i + 1) % 2) + last
    return (i + 1) // 2 - core * (1 - last) - last, core


def mixed_mask(part, v):
    code = v + (v + 5) // 8 - 2 * ((v + 4) // 8) + (v + 3) // 8
    m1, m2, m3 = (BIT[axis] for axis in MIXED_ORDER[part])
    return (code % 2) * m1 + ((code // 2) % 2) * m2 + (code // 4) * m3


def flip(bit, by):
    return bit + by - 2 * bit * by


def kernel(a_hbm, x_hbm, w1_hbm, w2_hbm, y_hbm, m_hbm, d1out, d2out,
           abuf, xin, w1_ref, w2_ref, y_ref, m_ref, xall, hall, s1acc, s2acc, s1b, s2b, z1t, w1p, w1t, w2t, ut,
           acc, drecv, rbuf, gt,
           cnt, d2src, d2r1, d2r2, d1src, d1r1, d1r2,
           asem, xsem, gr, dr, rr, er, pr, snd):
    me = lax.axis_index(AXIS)
    core, px, py, pz = me % 2, (me // 2) % 2, (me // 4) % 2, me // 8

    def dev(mask, other=0):
        fx, fy, fz, fc = mask % 2, (mask // 2) % 2, mask // 4, other
        return ((flip(pz, fz) * 2 + flip(py, fy)) * 2 + flip(px, fx)) * 2 + flip(core, fc)

    def block_of(i):
        mask, other = step_order(i)
        return dev(mask, other)

    def load_a(i, slot):
        start = pl.multiple_of(block_of(i) * BLK, BLK)
        return pltpu.make_async_copy(a_hbm.at[:, pl.ds(start, BLK)], abuf.at[slot], asem.at[slot])

    def load_mixed(i, slot):
        v, other = mixed_order(i)
        for part, (start, size) in enumerate(MIXED_COLS):
            begin = pl.multiple_of(dev(mixed_mask(part, v), other) * BLK + start, 128)
            pltpu.make_async_copy(a_hbm.at[:, pl.ds(begin, size)], abuf.at[slot, :, pl.ds(start, size)],
                                  asem.at[slot]).start()

    def wait_a(slot):
        pltpu.make_async_copy(a_hbm.at[:, pl.ds(0, BLK)], abuf.at[slot], asem.at[slot]).wait()

    twin = dev(0, 1)

    def remote(src, dst, send, recv, to):
        return pltpu.make_async_remote_copy(src_ref=src, dst_ref=dst, send_sem=send, recv_sem=recv,
                                            device_id=(to,), device_id_type=MESH)

    def peer(d):
        return dev(d // 2, d % 2)

    far_first = sorted(range(1, NDEV), key=lambda d: -bin(d // 2).count('1'))

    barrier = pltpu.get_barrier_semaphore()
    for d in (8, 4, 2, 1):
        pl.semaphore_signal(barrier, inc=1, device_id=(peer(d),), device_id_type=MESH)
    loads = [pltpu.make_async_copy(src, dst, xsem.at[k]) for k, (src, dst) in enumerate((
        (x_hbm, xin), (m_hbm, m_ref), (w1_hbm, w1_ref), (w2_hbm, w2_ref), (y_hbm, y_ref)))]
    for load in loads:
        load.start()
    for i in range(RING):
        load_mixed(i, i)
    xall[0] = jnp.zeros((FROWS, BLK), BF16)
    loads[0].wait()
    xall[0, 0:FIN, :] = xin[...]
    loads[1].wait()
    cnt[me] = jnp.full((1, 128), jnp.sum(m_ref[...].astype(F32)), F32)
    pl.semaphore_wait(barrier, 4)

    def mixed_copy(part, slot):
        axis, cols = MIXED_ORDER[part][VIA[slot]], pl.ds(*MIXED_COLS[part])
        return remote(xall.at[SOURCE[slot], :, cols], xall.at[slot + 1, :, cols], snd.at[0], gr.at[slot], dev(BIT[axis]))

    def mixed_start(*slots):
        for slot in slots:
            for part in range(4):
                mixed_copy(part, slot).start()

    def mixed_give(v):
        remote(xall.at[v], xall.at[8 + v], snd.at[0], dr.at[v], twin).start()

    def mixed_take(sems, n):
        remote(xall.at[0], xall.at[0], snd.at[0], sems.at[n], me).wait_recv()

    def mixed_product(i):
        v, other = mixed_order(i)
        return lax.dot_general(xall[8 * other + v], abuf[i % RING], NT, preferred_element_type=F32)

    def mixed_refill(i):
        @pl.when(i < NDEV - RING)
        def _():
            load_mixed(i + RING, i % RING)

        @pl.when(i >= NDEV - RING)
        def _():
            load_a(i + RING - NDEV, i % RING).start()

    def aggregate_features():
        wait_a(0)
        s1acc[0:FROWS, :] += mixed_product(0)
        mixed_refill(0)

        @pl.loop(0, 7)
        def _(slot):
            for k in range(7):
                @pl.when(slot == k)
                def _():
                    mixed_take(gr, k)
                    mixed_start(*(later for later in range(3, 7) if SOURCE[later] == k + 1))
                    mixed_give(k + 1)
            mixed_take(dr, slot)
            i = 2 * slot + 1
            wait_a(i % RING)
            wait_a((i + 1) % RING)
            s1acc[0:FROWS, :] += mixed_product(i) + mixed_product(i + 1)
            mixed_refill(i)
            mixed_refill(i + 1)

        mixed_take(dr, 7)
        wait_a((NDEV - 1) % RING)
        s1acc[0:FROWS, :] += mixed_product(NDEV - 1)
        mixed_refill(NDEV - 1)

    def gather(buf, g):
        def piece(owner, part):
            return buf.at[owner, pl.ds(*GATHER_ROWS[part])]

        def copy(axis, slot):
            part, mask = gather_unit(axis, slot)
            ref = piece(dev(mask), part)
            n = 7 + (slot if slot < 4 else 4 if slot == 6 else 2 * axis + slot + 1)
            return remote(ref, ref, snd.at[g], gr.at[n], dev(BIT[axis]))

        def whole(sems, n):
            return remote(buf.at[me], buf.at[me], snd.at[g], sems.at[n], me)

        def give(*masks):
            for mask in masks:
                owner = dev(mask)
                for ref in [buf.at[owner]] if mask < 7 else [piece(owner, part) for part in AXES]:
                    remote(ref, ref, snd.at[g], dr.at[8 + mask], twin).start()

        def take(*masks):
            for mask in masks:
                whole(dr, 8 + mask).wait_recv()

        def begin():
            for slot in AXES:
                for axis in AXES:
                    copy(axis, slot).start()
            give(0)

        def forward(axis, slot, *onto):
            part, mask = gather_unit(axis, slot)
            for over, later in onto:
                assert gather_unit(over, later) == (part, mask | BIT[axis])
                copy(over, later).start()

        def arrive(*slots):
            for slot in slots:
                whole(gr, 7 + min(slot, 4)).wait_recv()

        def arrive_one(axis, slot):
            part, mask = gather_unit(axis, slot)
            ref = piece(dev(mask | BIT[axis]), part)
            remote(ref, ref, snd.at[g], gr.at[8 + 2 * axis + slot], me).wait_recv()

        def hooks(p):
            @pl.when(p == 0)
            def _():
                take(0)

            @pl.when(p == 1)
            def _():
                for slot in AXES:
                    arrive(slot)
                    for over in AXES:
                        if slot == 0:
                            forward((over + 2) % 3, 0, (over, 3))
                        if slot == 1:
                            forward((over + 2) % 3, 1, (over, 5))
                        if (slot == 0) == (over != 1) and slot < 2:
                            forward((over + 1) % 3, 0, (over, 4))
                give(1, 2, 4)

            @pl.when(p == 2)
            def _():
                take(1)

            @pl.when(p == 3)
            def _():
                take(2, 4)

            @pl.when(p == 4)
            def _():
                arrive(3)
                for over in AXES:
                    forward((over + 2) % 3, 3, (over, 6))
                arrive_one(1, 5)
                arrive_one(0, 4)
                give(3)
                take(3)

            @pl.when(p == 5)
            def _():
                arrive_one(2, 4)
                arrive_one(1, 4)
                arrive_one(0, 5)
                arrive_one(2, 5)
                give(5, 6)

            @pl.when(p == 6)
            def _():
                take(5, 6)

        def tail(i):
            @pl.when(i == 0)
            def _():
                arrive(6)
                give(7)

            @pl.when(i == 1)
            def _():
                take(7)

        return begin, hooks, tail

    def drain(buf, n):
        every = buf.at[pl.ds(0, 15)]
        remote(every, every, snd.at[n], gr.at[n], me).wait_send()

    def aggregate(buf, total, hooks, tail):
        def product(i):
            return jnp.dot(abuf[(NDEV + i) % RING], buf[block_of(i)], preferred_element_type=F32)

        def refill(i):
            @pl.when(i < NDEV - RING)
            def _():
                load_a(i + RING, (NDEV + i) % RING).start()

        @pl.loop(0, 7)
        def _(p):
            hooks(p)
            for k in BOTH:
                wait_a((NDEV + 2 * p + k) % RING)
            total[...] += product(2 * p) + product(2 * p + 1)
            for k in BOTH:
                refill(2 * p + k)

        @pl.loop(0, 2)
        def _(k):
            tail(k)
            wait_a((NDEV + 14 + k) % RING)
            total[...] += product(14 + k)

    def small(x, src, dst, scatter=False):
        for d in far_first:
            remote(src.at[peer(d)] if scatter else src, dst.at[me], snd.at[3 + x], pr.at[x], peer(d)).start()

    def small_wait(x, dst):
        ref = dst.at[pl.ds(0, 15)]
        remote(ref, ref, snd.at[3 + x], pr.at[x], me).wait()

    begin_h, hooks_h, tail_h = gather(hall, 1)

    mixed_start(0, 1, 2)
    mixed_give(0)
    for load in loads[2:]:
        load.wait()
    w1p[...] = jnp.zeros_like(w1p)
    w1p[0:FIN, :] = w1_ref[...]
    w1t[...] = w1p[...].T.astype(BF16)
    w2t[...] = jnp.zeros_like(w2t)
    w2t[0:NCLS, :] = w2_ref[...].astype(BF16)
    s1acc[...] = jnp.zeros_like(s1acc)
    s2acc[...] = jnp.zeros_like(s2acc)
    aggregate_features()

    s1b[...] = s1acc[...].astype(BF16)
    pre_one = jnp.dot(s1acc[...].T.astype(BF16), w1p[...].astype(BF16), preferred_element_type=F32)
    hall[me] = jnp.maximum(pre_one, 0.0).astype(BF16)
    begin_h()
    small(0, cnt.at[me], cnt)
    z1t[...] = jnp.dot(w1t[...], s1b[...], preferred_element_type=F32)
    aggregate(hall, s2acc, hooks_h, tail_h)

    small_wait(0, cnt)
    label_count = jnp.sum(cnt[...], axis=0)[0:1, 0:1]
    s2b[...] = s2acc[...].astype(BF16)
    logits = lax.dot_general(w2t[...], s2b[...], NT, preferred_element_type=F32)
    classes = lax.broadcasted_iota(jnp.int32, (CPAD, BLK), 0)
    logits = jnp.where(classes < NCLS, logits, -jnp.inf)
    shifted = logits - jnp.max(logits, axis=0, keepdims=True)
    log_prob = shifted - jnp.log(jnp.sum(jnp.exp(shifted), axis=0, keepdims=True))
    hit = classes == y_ref[...]
    weight = m_ref[...].astype(F32)
    picked = jnp.sum(jnp.where(hit, log_prob, 0.0), axis=0, keepdims=True)
    loss_part = -jnp.sum(weight * picked)
    grad = weight * (jnp.exp(log_prob) - jnp.where(hit, 1.0, 0.0)) / label_count
    gt[...] = grad.astype(BF16)
    ut[...] = lax.dot_general(w2t[...], gt[...], TN, preferred_element_type=F32).astype(BF16)

    def pair_sum(mask, half=None):
        if half is None:
            return remote(acc.at[8 + mask], drecv.at[mask], snd.at[2], er.at[mask], twin)
        cols = pl.ds(half * 512, 512)
        return remote(acc.at[8 + mask, :, cols], drecv.at[mask, :, cols], snd.at[2], er.at[mask + half],
                      twin)

    def unit_copy(part, k, half=None):
        axis, mask = reduce_unit(part, k)
        rows = pl.ds(*REDUCE_ROWS[part])
        if half is None:
            return remote(acc.at[mask, rows], rbuf.at[k, rows], snd.at[2], rr.at[k], dev(BIT[axis]))
        cols = pl.ds(half * 512, 512)
        return remote(acc.at[mask, rows, cols], rbuf.at[k, rows, cols], snd.at[2], rr.at[k], dev(BIT[axis]))

    def add_rows(mask, source, start, size, cols=slice(None)):
        @pl.loop(0, size // 8)
        def _(t):
            rows = pl.ds(pl.multiple_of(start + t * 8, 8), 8)
            acc[mask, rows, cols] += source[rows, cols]

    def take_pair(mask):
        pair_sum(mask).wait_recv()
        add_rows(mask, drecv.at[mask], 0, HID)
        for k in range(1, 4):
            for part in AXES:
                if reduce_unit(part, k)[1] == mask:
                    unit_copy(part, k).start()

    @pl.loop(0, 4)
    def _(q):
        other, half = 1 - q // 2, q % 2
        cols = pl.ds(pl.multiple_of(half * 512, 512), 512)
        acc[7 + 8 * other, :, cols] = jnp.dot(ut[...], abuf[(30 + other) % RING, :, cols], preferred_element_type=F32)
        for half in BOTH:
            @pl.when(q == half)
            def _():
                pair_sum(7, half).start()

    for j in BOTH:
        load_a(NDEV - 1 - j - RING, (31 - j) % RING).start()

    for half in BOTH:
        pair_sum(7, half).wait_recv()
        add_rows(7, drecv.at[7], 0, HID, pl.ds(half * 512, 512))
        for part in AXES:
            unit_copy(part, 0, half).start()

    @pl.loop(1, 8)
    def _(p):
        for k in BOTH:
            @pl.when(p >= 3)
            def _():
                wait_a((31 - 2 * p - k) % RING)
        for k in BOTH:
            mask, other = step_order(NDEV - 1 - 2 * p - k)
            acc[mask + 8 * other] = jnp.dot(ut[...], abuf[(31 - 2 * p - k) % RING], preferred_element_type=F32)
        for k in BOTH:
            @pl.when(p < 5)
            def _():
                load_a(NDEV - 1 - 2 * p - k - RING, (31 - 2 * p - k) % RING).start()

        for step in range(2, NDEV):
            step_mask, step_other = step_order(NDEV - 1 - step)

            @pl.when(p == step // 2)
            def _():
                if step_other:
                    pair_sum(step_mask).start()
                else:
                    take_pair(step_mask)

    def units_wait(k):
        remote(rbuf.at[k], rbuf.at[k], snd.at[2], rr.at[k], me).wait_recv()

    def take_units(k, send=None):
        units_wait(k)
        for part in AXES:
            axis, mask = reduce_unit(part, k)
            add_rows(mask - BIT[axis], rbuf.at[k], *REDUCE_ROWS[part])
            if send is not None:
                unit_copy(part, send).start()

    take_units(0, 4)
    take_units(1, 5)
    take_units(2)
    take_units(3)
    take_units(4, 6)
    dw2_part = jnp.dot(gt[...], s2b[...], preferred_element_type=F32)
    d2src[...] = jnp.zeros_like(d2src)
    for j in range(6):
        for k in BOTH:
            d2src[6 * k + j] = dw2_part[j * 8:(j + 1) * 8, k * 128:(k + 1) * 128]
    d2src[12] = jnp.full(TILE, loss_part, F32)
    d2src[13] = jnp.full(TILE, jnp.sum(weight), F32)
    keep_two = pltpu.make_async_copy(d2r2, d2out.at[me], xsem.at[0])
    d2r1[me] = d2src[me]
    small(1, d2src, d2r1, True)
    take_units(5)
    units_wait(6)
    grad_one = jnp.where(z1t[...] > 0.0, acc[0] + rbuf[6], 0.0).astype(BF16)
    d1src[...] = lax.dot_general(grad_one, s1b[...], NT, preferred_element_type=F32).reshape(NDEV, 16, FPAD)
    d1r1[me] = d1src[me]
    small(3, d1src, d1r1, True)
    small_wait(1, d2r1)
    d2r2[...] = jnp.sum(d2r1[...], axis=0)
    small(2, d2r2, d2out)
    keep_two.start()
    for n, buf in enumerate((xall, hall, acc)):
        drain(buf, n)
    small_wait(3, d1r1)
    d1r2[...] = jnp.sum(d1r1[...], axis=0)
    small(4, d1r2, d1out)
    keep_one = pltpu.make_async_copy(d1r2, d1out.at[me], xsem.at[1])
    keep_one.start()
    small_wait(2, d2out)
    keep_two.wait()
    keep_one.wait()
    small_wait(4, d1out)


def finish(d1_ref, d2_ref, loss_out, dw1_out, dw2_out):
    loss_out[...] = d2_ref[12, 0:1, 0:1] / d2_ref[13, 0:1, 0:1]
    dw1_out[...] = d1_ref[...].reshape(HID, FPAD).T[0:FIN, :]
    for k in BOTH:
        dw2_out[:, pl.ds(k * 128, 128)] = d2_ref[pl.ds(6 * k, 6)].reshape(CPAD, 128)[0:NCLS]


def solution(mesh):
    def local_step(adj_rows, feat_rows, w_one, w_two, label_rows, mask_rows):
        vmem = pl.BlockSpec(memory_space=pltpu.VMEM)
        hbm = pl.BlockSpec(memory_space=pl.ANY)
        dma = pltpu.SemaphoreType.DMA
        parts = pl.pallas_call(
            kernel,
            out_shape=(jax.ShapeDtypeStruct((NDEV, 16, FPAD), F32), jax.ShapeDtypeStruct((NDEV, *TILE), F32)),
            in_specs=[hbm] * 6,
            out_specs=(hbm, hbm),
            scratch_shapes=[
                pltpu.VMEM((RING, BLK, BLK), BF16),
                pltpu.VMEM((FIN, BLK), BF16),
                pltpu.VMEM((FIN, HID), F32),
                pltpu.VMEM((NCLS, HID), F32),
                pltpu.VMEM((1, BLK), jnp.int32),
                pltpu.VMEM((1, BLK), jnp.int32),
                pltpu.VMEM((NDEV, FROWS, BLK), BF16),
                pltpu.VMEM((NDEV, BLK, HID), BF16),
                pltpu.VMEM((FPAD, BLK), F32),
                pltpu.VMEM((BLK, HID), F32),
                pltpu.VMEM((FPAD, BLK), BF16),
                pltpu.VMEM((BLK, HID), BF16),
                pltpu.VMEM((HID, BLK), F32),
                pltpu.VMEM((FPAD, HID), F32),
                pltpu.VMEM((HID, FPAD), BF16),
                pltpu.VMEM((CPAD, HID), BF16),
                pltpu.VMEM((HID, BLK), BF16),
                pltpu.VMEM((16, HID, BLK), F32),
                pltpu.VMEM((8, HID, BLK), F32),
                pltpu.VMEM((7, HID, BLK), F32),
                pltpu.VMEM((CPAD, BLK), BF16),
                pltpu.VMEM((NDEV, 1, 128), F32),
                *[pltpu.VMEM((NDEV, *TILE), F32)] * 2,
                pltpu.VMEM(TILE, F32),
                *[pltpu.VMEM((NDEV, 16, FPAD), F32)] * 2,
                pltpu.VMEM((16, FPAD), F32),
                *[dma((n,)) for n in (RING, 5, 18, 16, 7, 9, 5, 8)],
            ],
            compiler_params=pltpu.CompilerParams(collective_id=0, has_side_effects=True,
                                                 vmem_limit_bytes=67 * 1000 * 1000),
        )(adj_rows, feat_rows.T, w_one, w_two.T, label_rows.reshape(1, BLK), mask_rows.reshape(1, BLK))
        loss, dw_one, dw_two = pl.pallas_call(
            finish,
            out_shape=(jax.ShapeDtypeStruct((1, 1), F32), jax.ShapeDtypeStruct((FIN, HID), F32),
                       jax.ShapeDtypeStruct((NCLS, HID), F32)),
            in_specs=[vmem] * 2,
            out_specs=(vmem, vmem, vmem),
        )(*parts)
        return loss.reshape(1), dw_one, dw_two.T

    return jax.shard_map(local_step, mesh=mesh,
                         in_specs=(P(AXIS, None), P(AXIS, None), P(None, None), P(None, None), P(AXIS), P(AXIS)),
                         out_specs=(P(None), P(None, None), P(None, None)), check_vma=False)
```

```python
import functools

import jax
import jax.numpy as jnp
from jax import lax
from jax.experimental import pallas as pl
from jax.experimental.pallas import tpu as pltpu
from jax.sharding import PartitionSpec as P

MESH = pl.DeviceIdType.MESH
AXIS = 'nodes'
F32, BF16 = jnp.float32, jnp.bfloat16
NDEV = 16
BLK = 1024
FIN, FROWS, FPAD = 100, 104, 128
HID = 256
NCLS, CPAD = 47, 48
RING = 6
TILE = (8, 128)

AXES, BOTH, QUARTERS = range(3), range(2), range(4)
BIT = (1, 2, 4)
ORDER = tuple((p, (p + 1) % 3, (p + 2) % 3) for p in AXES)
GATHER_ROWS = ((0, 352), (352, 336), (688, 336))
MIXED_COLS = ((0, 384), (384, 384), (768, 256))
REDUCE_ROWS = ((0, 88), (88, 88), (176, 80))

NT = (((1,), (1,)), ((), ()))
TN = (((0,), (0,)), ((), ()))


CODE = (0, 1, 2, 4, 3, 5, 6, 7)
VIA = [code.bit_length() - 1 for code in CODE[1:]]
SOURCE = [CODE.index(code - (1 << via)) for code, via in zip(CODE[1:], VIA)]


def gather_unit(axis, slot):
    part = next(p for p in AXES if ORDER[p][VIA[slot]] == axis)
    return part, sum(BIT[ORDER[part][j]] for j in AXES if CODE[SOURCE[slot]] >> j & 1)


def reduce_unit(part, k):
    b1, b2, b3 = ORDER[part]
    m1, m2, m3 = BIT[b1], BIT[b2], BIT[b3]
    return ((b1, m1 | m2 | m3), (b1, m1 | m2), (b1, m1 | m3), (b1, m1), (b2, m2 | m3), (b2, m2), (b3, m3))[k]


def step_order(i):
    from2, from8, from10, from14 = ((i + 16 - n) // 16 for n in (2, 8, 10, 14))
    j = (i + 1) % 3
    one, xy, two = from2 - from8, from8 - from10, from10 - from14
    mask = one * ((j * j + j + 2) // 2) + xy * 3 + two * (5 + i % 2) + from14 * 7
    core = (1 - from2) * i + one * ((i + 1) // 3 - 1) + xy * (i - 8) + two * (i // 2 - 5) + from14 * (i - 14)
    return mask, core


def mixed_order(i):
    first, last = 1 - (i + 15) // 16, i // 15
    core = (1 - first) * (1 - last) * ((i + 1) % 2) + last
    return (i + 1) // 2 - core * (1 - last) - last, core


def mixed_mask(part, v):
    code = v + (v + 5) // 8 - 2 * ((v + 4) // 8) + (v + 3) // 8
    m1, m2, m3 = (BIT[axis] for axis in ORDER[part])
    return (code % 2) * m1 + ((code // 2) % 2) * m2 + (code // 4) * m3


def flip(bit, by):
    return bit + by - 2 * bit * by


def kernel(a_hbm, x_hbm, w1_hbm, w2_hbm, y_hbm, m_hbm, d1out, d2out,
           abuf, xin, w1_ref, w2_ref, y_ref, m_ref, xall, hall, s1acc, s2acc, s1b, s2b, z1t, w1p, w1t, w2t, ut,
           acc, drecv, rbuf, gt,
           cnt, d2src, d2r1, d2r2, d1src, d1r1, d1r2,
           asem, xsem, gr, dr, rr, er, pr, snd):
    me = lax.axis_index(AXIS)
    core, px, py, pz = me % 2, (me // 2) % 2, (me // 4) % 2, me // 8

    def dev(mask, other=0):
        fx, fy, fz, fc = mask % 2, (mask // 2) % 2, mask // 4, other
        return ((flip(pz, fz) * 2 + flip(py, fy)) * 2 + flip(px, fx)) * 2 + flip(core, fc)

    def block_of(i):
        mask, other = step_order(i)
        return dev(mask, other)

    def load_a(i, slot):
        start = pl.multiple_of(block_of(i) * BLK, BLK)
        return pltpu.make_async_copy(a_hbm.at[:, pl.ds(start, BLK)], abuf.at[slot], asem.at[slot])

    def load_mixed(i, slot):
        v, other = mixed_order(i)
        for part, (start, size) in enumerate(MIXED_COLS):
            begin = pl.multiple_of(dev(mixed_mask(part, v), other) * BLK + start, 128)
            pltpu.make_async_copy(a_hbm.at[:, pl.ds(begin, size)], abuf.at[slot, :, pl.ds(start, size)],
                                  asem.at[slot]).start()

    def wait_a(slot):
        pltpu.make_async_copy(a_hbm.at[:, pl.ds(0, BLK)], abuf.at[slot], asem.at[slot]).wait()

    twin = dev(0, 1)

    def remote(src, dst, send, recv, to):
        return pltpu.make_async_remote_copy(src_ref=src, dst_ref=dst, send_sem=send, recv_sem=recv,
                                            device_id=(to,), device_id_type=MESH)

    def peer(d):
        return dev(d // 2, d % 2)

    far_first = sorted(range(1, NDEV), key=lambda d: -bin(d // 2).count('1'))

    barrier = pltpu.get_barrier_semaphore()
    for d in (8, 4, 2, 1):
        pl.semaphore_signal(barrier, inc=1, device_id=(peer(d),), device_id_type=MESH)
    loads = [pltpu.make_async_copy(src, dst, xsem.at[k]) for k, (src, dst) in enumerate((
        (x_hbm, xin), (m_hbm, m_ref), (w1_hbm, w1_ref), (w2_hbm, w2_ref), (y_hbm, y_ref)))]
    for load in loads:
        load.start()
    for i in range(RING):
        load_mixed(i, i)
    xall[0] = jnp.zeros((FROWS, BLK), BF16)
    loads[0].wait()
    xall[0, 0:FIN, :] = xin[...]
    loads[1].wait()
    cnt[me] = jnp.full((1, 128), jnp.sum(m_ref[...].astype(F32)), F32)
    pl.semaphore_wait(barrier, 4)

    def mixed_copy(part, slot):
        axis, cols = ORDER[part][VIA[slot]], pl.ds(*MIXED_COLS[part])
        return remote(xall.at[SOURCE[slot], :, cols], xall.at[slot + 1, :, cols], snd.at[0], gr.at[slot], dev(BIT[axis]))

    def mixed_start(*slots):
        for slot in slots:
            for part in AXES:
                mixed_copy(part, slot).start()

    def mixed_give(v):
        remote(xall.at[v], xall.at[8 + v], snd.at[0], dr.at[v], twin).start()

    def mixed_take(sems, n):
        remote(xall.at[0], xall.at[0], snd.at[0], sems.at[n], me).wait_recv()

    def mixed_product(i):
        v, other = mixed_order(i)
        return lax.dot_general(xall[8 * other + v], abuf[i % RING], NT, preferred_element_type=F32)

    def mixed_refill(i):
        @pl.when(i < NDEV - RING)
        def _():
            load_mixed(i + RING, i % RING)

        @pl.when(i >= NDEV - RING)
        def _():
            load_a(i + RING - NDEV, i % RING).start()

    def aggregate_features():
        wait_a(0)
        s1acc[0:FROWS, :] += mixed_product(0)
        mixed_refill(0)

        @pl.loop(0, 7)
        def _(slot):
            for k in range(7):
                @pl.when(slot == k)
                def _():
                    mixed_take(gr, k)
                    mixed_start(*(later for later in range(3, 7) if SOURCE[later] == k + 1))
                    mixed_give(k + 1)
            mixed_take(dr, slot)
            i = 2 * slot + 1
            wait_a(i % RING)
            wait_a((i + 1) % RING)
            s1acc[0:FROWS, :] += mixed_product(i) + mixed_product(i + 1)
            mixed_refill(i)
            mixed_refill(i + 1)

        mixed_take(dr, 7)
        wait_a((NDEV - 1) % RING)
        s1acc[0:FROWS, :] += mixed_product(NDEV - 1)
        mixed_refill(NDEV - 1)

    def gather(buf, g):
        def piece(owner, part):
            return buf.at[owner, pl.ds(*GATHER_ROWS[part])]

        def copy(axis, slot):
            part, mask = gather_unit(axis, slot)
            ref = piece(dev(mask), part)
            n = 7 + (slot if slot < 4 else 4 if slot == 6 else 2 * axis + slot + 1)
            return remote(ref, ref, snd.at[g], gr.at[n], dev(BIT[axis]))

        def whole(sems, n):
            return remote(buf.at[me], buf.at[me], snd.at[g], sems.at[n], me)

        def give(*masks):
            for mask in masks:
                owner = dev(mask)
                for ref in [buf.at[owner]] if mask < 7 else [piece(owner, part) for part in AXES]:
                    remote(ref, ref, snd.at[g], dr.at[8 + mask], twin).start()

        def take(*masks):
            for mask in masks:
                whole(dr, 8 + mask).wait_recv()

        def begin():
            for slot in AXES:
                for axis in AXES:
                    copy(axis, slot).start()
            give(0)

        def forward(axis, slot, *onto):
            part, mask = gather_unit(axis, slot)
            for over, later in onto:
                assert gather_unit(over, later) == (part, mask | BIT[axis])
                copy(over, later).start()

        def arrive(*slots):
            for slot in slots:
                whole(gr, 7 + min(slot, 4)).wait_recv()

        def arrive_one(axis, slot):
            part, mask = gather_unit(axis, slot)
            ref = piece(dev(mask | BIT[axis]), part)
            remote(ref, ref, snd.at[g], gr.at[8 + 2 * axis + slot], me).wait_recv()

        def hooks(p):
            @pl.when(p == 0)
            def _():
                take(0)

            @pl.when(p == 1)
            def _():
                for slot in AXES:
                    arrive(slot)
                    for over in AXES:
                        if slot == 0:
                            forward((over + 2) % 3, 0, (over, 3))
                        if slot == 1:
                            forward((over + 2) % 3, 1, (over, 5))
                        if (slot == 0) == (over != 1) and slot < 2:
                            forward((over + 1) % 3, 0, (over, 4))
                give(1, 2, 4)

            @pl.when(p == 2)
            def _():
                take(1)

            @pl.when(p == 3)
            def _():
                take(2, 4)

            @pl.when(p == 4)
            def _():
                arrive(3)
                for over in AXES:
                    forward((over + 2) % 3, 3, (over, 6))
                arrive_one(1, 5)
                arrive_one(0, 4)
                give(3)
                take(3)

            @pl.when(p == 5)
            def _():
                arrive_one(2, 4)
                arrive_one(1, 4)
                arrive_one(0, 5)
                arrive_one(2, 5)
                give(5, 6)

            @pl.when(p == 6)
            def _():
                take(5, 6)

        def tail(i):
            @pl.when(i == 0)
            def _():
                arrive(6)
                give(7)

            @pl.when(i == 1)
            def _():
                take(7)

        return begin, hooks, tail

    def drain(buf, n):
        every = buf.at[pl.ds(0, 15)]
        remote(every, every, snd.at[n], gr.at[n], me).wait_send()

    def aggregate(buf, total, hooks, tail):
        def product(i):
            return jnp.dot(abuf[(NDEV + i) % RING], buf[block_of(i)], preferred_element_type=F32)

        def refill(i):
            @pl.when(i < NDEV - RING)
            def _():
                load_a(i + RING, (NDEV + i) % RING).start()

        @pl.loop(0, 7)
        def _(p):
            hooks(p)
            for k in BOTH:
                wait_a((NDEV + 2 * p + k) % RING)
            total[...] += product(2 * p) + product(2 * p + 1)
            for k in BOTH:
                refill(2 * p + k)

        @pl.loop(0, 2)
        def _(k):
            tail(k)
            wait_a((NDEV + 14 + k) % RING)
            total[...] += product(14 + k)

    def small(x, src, dst, scatter=False):
        for d in far_first:
            remote(src.at[peer(d)] if scatter else src, dst.at[me], snd.at[3 + x], pr.at[x], peer(d)).start()

    def small_wait(x, dst):
        ref = dst.at[pl.ds(0, 15)]
        remote(ref, ref, snd.at[3 + x], pr.at[x], me).wait()

    begin_h, hooks_h, tail_h = gather(hall, 1)

    mixed_start(0, 1, 2)
    mixed_give(0)
    for load in loads[2:]:
        load.wait()
    w1p[...] = jnp.zeros_like(w1p)
    w1p[0:FIN, :] = w1_ref[...]
    w1t[...] = w1p[...].T.astype(BF16)
    w2t[...] = jnp.zeros_like(w2t)
    w2t[0:NCLS, :] = w2_ref[...].astype(BF16)
    s1acc[...] = jnp.zeros_like(s1acc)
    s2acc[...] = jnp.zeros_like(s2acc)
    aggregate_features()

    s1b[...] = s1acc[...].astype(BF16)
    pre_one = jnp.dot(s1acc[...].T.astype(BF16), w1p[...].astype(BF16), preferred_element_type=F32)
    hall[me] = jnp.maximum(pre_one, 0.0).astype(BF16)
    begin_h()
    small(0, cnt.at[me], cnt)
    z1t[...] = jnp.dot(w1t[...], s1b[...], preferred_element_type=F32)
    aggregate(hall, s2acc, hooks_h, tail_h)

    small_wait(0, cnt)
    label_count = jnp.sum(cnt[...], axis=0)[0:1, 0:1]
    s2b[...] = s2acc[...].astype(BF16)
    logits = lax.dot_general(w2t[...], s2b[...], NT, preferred_element_type=F32)
    classes = lax.broadcasted_iota(jnp.int32, (CPAD, BLK), 0)
    logits = jnp.where(classes < NCLS, logits, -jnp.inf)
    shifted = logits - jnp.max(logits, axis=0, keepdims=True)
    log_prob = shifted - jnp.log(jnp.sum(jnp.exp(shifted), axis=0, keepdims=True))
    hit = classes == y_ref[...]
    weight = m_ref[...].astype(F32)
    picked = jnp.sum(jnp.where(hit, log_prob, 0.0), axis=0, keepdims=True)
    loss_part = -jnp.sum(weight * picked)
    grad = weight * (jnp.exp(log_prob) - jnp.where(hit, 1.0, 0.0)) / label_count
    gt[...] = grad.astype(BF16)
    ut[...] = lax.dot_general(w2t[...], gt[...], TN, preferred_element_type=F32).astype(BF16)

    def pair_sum(mask, quarter=None):
        if quarter is None:
            return remote(acc.at[8 + mask], drecv.at[mask], snd.at[2], er.at[mask], twin)
        cols = pl.ds(quarter * 256, 256)
        return remote(acc.at[8 + mask, :, cols], drecv.at[mask, :, cols], snd.at[2], er.at[mask + quarter],
                      twin)

    def unit_copy(part, k, quarter=None):
        axis, mask = reduce_unit(part, k)
        rows = pl.ds(*REDUCE_ROWS[part])
        if quarter is None:
            return remote(acc.at[mask, rows], rbuf.at[k, rows], snd.at[2], rr.at[k], dev(BIT[axis]))
        cols = pl.ds(quarter * 256, 256)
        return remote(acc.at[mask, rows, cols], rbuf.at[k, rows, cols], snd.at[2], rr.at[k], dev(BIT[axis]))

    def add_rows(mask, source, start, size, cols=slice(None)):
        @pl.loop(0, size // 8)
        def _(t):
            rows = pl.ds(pl.multiple_of(start + t * 8, 8), 8)
            acc[mask, rows, cols] += source[rows, cols]

    def take_pair(mask):
        pair_sum(mask).wait_recv()
        add_rows(mask, drecv.at[mask], 0, HID)
        for k in range(1, 4):
            for part in AXES:
                if reduce_unit(part, k)[1] == mask:
                    unit_copy(part, k).start()

    for other in (1, 0):
        for q in QUARTERS:
            cols = pl.ds(q * 256, 256)
            acc[7 + 8 * other, :, cols] = jnp.dot(ut[...], abuf[(30 + other) % RING, :, cols],
                                                  preferred_element_type=F32)
            if other:
                pair_sum(7, q).start()

    for j in BOTH:
        load_a(NDEV - 1 - j - RING, (31 - j) % RING).start()

    for q in QUARTERS:
        pair_sum(7, q).wait_recv()
        cols = pl.ds(q * 256, 256)
        acc[7, :, cols] += drecv[7, :, cols]
        for part in AXES:
            unit_copy(part, 0, q).start()

    @pl.loop(1, 8)
    def _(p):
        for k in BOTH:
            @pl.when(p >= 3)
            def _():
                wait_a((31 - 2 * p - k) % RING)
        for k in BOTH:
            mask, other = step_order(NDEV - 1 - 2 * p - k)
            acc[mask + 8 * other] = jnp.dot(ut[...], abuf[(31 - 2 * p - k) % RING], preferred_element_type=F32)
        for k in BOTH:
            @pl.when(p < 5)
            def _():
                load_a(NDEV - 1 - 2 * p - k - RING, (31 - 2 * p - k) % RING).start()

        for step in range(2, NDEV):
            step_mask, step_other = step_order(NDEV - 1 - step)

            @pl.when(p == step // 2)
            def _():
                if step_other:
                    pair_sum(step_mask).start()
                else:
                    take_pair(step_mask)

    def units_wait(k):
        remote(rbuf.at[k], rbuf.at[k], snd.at[2], rr.at[k], me).wait_recv()

    def take_units(k, send=None):
        units_wait(k)
        for part in AXES:
            axis, mask = reduce_unit(part, k)
            add_rows(mask - BIT[axis], rbuf.at[k], *REDUCE_ROWS[part])
            if send is not None:
                unit_copy(part, send).start()

    take_units(0, 4)
    take_units(1, 5)
    take_units(2)
    take_units(3)
    take_units(4, 6)
    dw2_part = jnp.dot(gt[...], s2b[...], preferred_element_type=F32)
    d2src[...] = jnp.zeros_like(d2src)
    for j in range(6):
        for k in BOTH:
            d2src[6 * k + j] = dw2_part[j * 8:(j + 1) * 8, k * 128:(k + 1) * 128]
    d2src[12] = jnp.full(TILE, loss_part, F32)
    d2src[13] = jnp.full(TILE, jnp.sum(weight), F32)
    keep_two = pltpu.make_async_copy(d2r2, d2out.at[me], xsem.at[0])
    d2r1[me] = d2src[me]
    small(1, d2src, d2r1, True)
    take_units(5)
    units_wait(6)
    grad_one = jnp.where(z1t[...] > 0.0, acc[0] + rbuf[6], 0.0).astype(BF16)
    d1src[...] = lax.dot_general(grad_one, s1b[...], NT, preferred_element_type=F32).reshape(NDEV, 16, FPAD)
    d1r1[me] = d1src[me]
    small(3, d1src, d1r1, True)
    small_wait(1, d2r1)
    d2r2[...] = jnp.sum(d2r1[...], axis=0)
    small(2, d2r2, d2out)
    keep_two.start()
    for n, buf in enumerate((xall, hall, acc)):
        drain(buf, n)
    small_wait(3, d1r1)
    d1r2[...] = jnp.sum(d1r1[...], axis=0)
    small(4, d1r2, d1out)
    keep_one = pltpu.make_async_copy(d1r2, d1out.at[me], xsem.at[1])
    keep_one.start()
    small_wait(2, d2out)
    keep_two.wait()
    keep_one.wait()
    small_wait(4, d1out)


def finish(d1_ref, d2_ref, loss_out, dw1_out, dw2_out):
    loss_out[...] = d2_ref[12, 0:1, 0:1] / d2_ref[13, 0:1, 0:1]
    dw1_out[...] = d1_ref[...].reshape(HID, FPAD).T[0:FIN, :]
    for k in BOTH:
        dw2_out[:, pl.ds(k * 128, 128)] = d2_ref[pl.ds(6 * k, 6)].reshape(CPAD, 128)[0:NCLS]


def solution(mesh):
    def local_step(adj_rows, feat_rows, w_one, w_two, label_rows, mask_rows):
        vmem = pl.BlockSpec(memory_space=pltpu.VMEM)
        hbm = pl.BlockSpec(memory_space=pl.ANY)
        dma = pltpu.SemaphoreType.DMA
        parts = pl.pallas_call(
            kernel,
            out_shape=(jax.ShapeDtypeStruct((NDEV, 16, FPAD), F32), jax.ShapeDtypeStruct((NDEV, *TILE), F32)),
            in_specs=[hbm] * 6,
            out_specs=(hbm, hbm),
            scratch_shapes=[
                pltpu.VMEM((RING, BLK, BLK), BF16),
                pltpu.VMEM((FIN, BLK), BF16),
                pltpu.VMEM((FIN, HID), F32),
                pltpu.VMEM((NCLS, HID), F32),
                pltpu.VMEM((1, BLK), jnp.int32),
                pltpu.VMEM((1, BLK), jnp.int32),
                pltpu.VMEM((NDEV, FROWS, BLK), BF16),
                pltpu.VMEM((NDEV, BLK, HID), BF16),
                pltpu.VMEM((FPAD, BLK), F32),
                pltpu.VMEM((BLK, HID), F32),
                pltpu.VMEM((FPAD, BLK), BF16),
                pltpu.VMEM((BLK, HID), BF16),
                pltpu.VMEM((HID, BLK), F32),
                pltpu.VMEM((FPAD, HID), F32),
                pltpu.VMEM((HID, FPAD), BF16),
                pltpu.VMEM((CPAD, HID), BF16),
                pltpu.VMEM((HID, BLK), BF16),
                pltpu.VMEM((16, HID, BLK), F32),
                pltpu.VMEM((8, HID, BLK), F32),
                pltpu.VMEM((7, HID, BLK), F32),
                pltpu.VMEM((CPAD, BLK), BF16),
                pltpu.VMEM((NDEV, 1, 128), F32),
                *[pltpu.VMEM((NDEV, *TILE), F32)] * 2,
                pltpu.VMEM(TILE, F32),
                *[pltpu.VMEM((NDEV, 16, FPAD), F32)] * 2,
                pltpu.VMEM((16, FPAD), F32),
                *[dma((n,)) for n in (RING, 5, 18, 16, 7, 11, 5, 8)],
            ],
            compiler_params=pltpu.CompilerParams(collective_id=0, has_side_effects=True,
                                                 vmem_limit_bytes=67 * 1000 * 1000),
        )(adj_rows, feat_rows.T, w_one, w_two.T, label_rows.reshape(1, BLK), mask_rows.reshape(1, BLK))
        loss, dw_one, dw_two = pl.pallas_call(
            finish,
            out_shape=(jax.ShapeDtypeStruct((1, 1), F32), jax.ShapeDtypeStruct((FIN, HID), F32),
                       jax.ShapeDtypeStruct((NCLS, HID), F32)),
            in_specs=[vmem] * 2,
            out_specs=(vmem, vmem, vmem),
        )(*parts)
        return loss.reshape(1), dw_one, dw_two.T

    return jax.shard_map(local_step, mesh=mesh,
                         in_specs=(P(AXIS, None), P(AXIS, None), P(None, None), P(None, None), P(AXIS), P(AXIS)),
                         out_specs=(P(None), P(None, None), P(None, None)), check_vma=False)
```

```python
import functools

import jax
import jax.numpy as jnp
from jax import lax
from jax.experimental import pallas as pl
from jax.experimental.pallas import tpu as pltpu
from jax.sharding import PartitionSpec as P

MESH = pl.DeviceIdType.MESH
AXIS = 'nodes'
F32, BF16 = jnp.float32, jnp.bfloat16
NDEV = 16
BLK = 1024
FIN, FROWS, FPAD = 100, 104, 128
HID = 256
NCLS, CPAD = 47, 48
RING = 6
TILE = (8, 128)

AXES, BOTH, QUARTERS = range(3), range(2), range(4)
BIT = (1, 2, 4)
ORDER = tuple((p, (p + 1) % 3, (p + 2) % 3) for p in AXES)
GATHER_ROWS = ((0, 352), (352, 336), (688, 336))
MIXED_COLS = ((0, 384), (384, 384), (768, 256))
REDUCE_ROWS = ((0, 88), (88, 88), (176, 80))

NT = (((1,), (1,)), ((), ()))
TN = (((0,), (0,)), ((), ()))


CODE = (0, 1, 2, 4, 3, 5, 6, 7)
VIA = [code.bit_length() - 1 for code in CODE[1:]]
SOURCE = [CODE.index(code - (1 << via)) for code, via in zip(CODE[1:], VIA)]


def gather_unit(axis, slot):
    part = next(p for p in AXES if ORDER[p][VIA[slot]] == axis)
    return part, sum(BIT[ORDER[part][j]] for j in AXES if CODE[SOURCE[slot]] >> j & 1)


def reduce_unit(part, k):
    b1, b2, b3 = ORDER[part]
    m1, m2, m3 = BIT[b1], BIT[b2], BIT[b3]
    return ((b1, m1 | m2 | m3), (b1, m1 | m2), (b1, m1 | m3), (b1, m1), (b2, m2 | m3), (b2, m2), (b3, m3))[k]


def step_order(i):
    from2, from8, from10, from14 = ((i + 16 - n) // 16 for n in (2, 8, 10, 14))
    j = (i + 1) % 3
    one, xy, two = from2 - from8, from8 - from10, from10 - from14
    mask = one * ((j * j + j + 2) // 2) + xy * 3 + two * (5 + i % 2) + from14 * 7
    core = (1 - from2) * i + one * ((i + 1) // 3 - 1) + xy * (i - 8) + two * (i // 2 - 5) + from14 * (i - 14)
    return mask, core


def mixed_order(i):
    first, last = 1 - (i + 15) // 16, i // 15
    core = (1 - first) * (1 - last) * ((i + 1) % 2) + last
    return (i + 1) // 2 - core * (1 - last) - last, core


def mixed_mask(part, v):
    code = v + (v + 5) // 8 - 2 * ((v + 4) // 8) + (v + 3) // 8
    m1, m2, m3 = (BIT[axis] for axis in ORDER[part])
    return (code % 2) * m1 + ((code // 2) % 2) * m2 + (code // 4) * m3


def flip(bit, by):
    return bit + by - 2 * bit * by


def kernel(a_hbm, x_hbm, w1_hbm, w2_hbm, y_hbm, m_hbm, d1out, d2out,
           abuf, xin, w1_ref, w2_ref, y_ref, m_ref, xall, hall, s1acc, s2acc, s1b, s2b, z1t, w1p, w1t, w2t, ut,
           acc, drecv, rbuf, gt,
           cnt, d2src, d2r1, d2r2, d1src, d1r1, d1r2,
           asem, xsem, gr, dr, rr, er, pr, snd):
    me = lax.axis_index(AXIS)
    core, px, py, pz = me % 2, (me // 2) % 2, (me // 4) % 2, me // 8

    def dev(mask, other=0):
        fx, fy, fz, fc = mask % 2, (mask // 2) % 2, mask // 4, other
        return ((flip(pz, fz) * 2 + flip(py, fy)) * 2 + flip(px, fx)) * 2 + flip(core, fc)

    def block_of(i):
        mask, other = step_order(i)
        return dev(mask, other)

    def load_a(i, slot):
        start = pl.multiple_of(block_of(i) * BLK, BLK)
        return pltpu.make_async_copy(a_hbm.at[:, pl.ds(start, BLK)], abuf.at[slot], asem.at[slot])

    def load_mixed(i, slot):
        v, other = mixed_order(i)
        for part, (start, size) in enumerate(MIXED_COLS):
            begin = pl.multiple_of(dev(mixed_mask(part, v), other) * BLK + start, 128)
            pltpu.make_async_copy(a_hbm.at[:, pl.ds(begin, size)], abuf.at[slot, :, pl.ds(start, size)],
                                  asem.at[slot]).start()

    def wait_a(slot):
        pltpu.make_async_copy(a_hbm.at[:, pl.ds(0, BLK)], abuf.at[slot], asem.at[slot]).wait()

    twin = dev(0, 1)

    def remote(src, dst, send, recv, to):
        return pltpu.make_async_remote_copy(src_ref=src, dst_ref=dst, send_sem=send, recv_sem=recv,
                                            device_id=(to,), device_id_type=MESH)

    def peer(d):
        return dev(d // 2, d % 2)

    far_first = sorted(range(1, NDEV), key=lambda d: -bin(d // 2).count('1'))

    barrier = pltpu.get_barrier_semaphore()
    for d in (8, 4, 2, 1):
        pl.semaphore_signal(barrier, inc=1, device_id=(peer(d),), device_id_type=MESH)
    loads = [pltpu.make_async_copy(src, dst, xsem.at[k]) for k, (src, dst) in enumerate((
        (x_hbm, xin), (m_hbm, m_ref), (w1_hbm, w1_ref), (w2_hbm, w2_ref), (y_hbm, y_ref)))]
    for load in loads:
        load.start()
    for i in range(RING):
        load_mixed(i, i)
    xall[0] = jnp.zeros((FROWS, BLK), BF16)
    loads[0].wait()
    xall[0, 0:FIN, :] = xin[...]
    loads[1].wait()
    cnt[me] = jnp.full((1, 128), jnp.sum(m_ref[...].astype(F32)), F32)
    pl.semaphore_wait(barrier, 4)

    def mixed_copy(part, slot):
        axis, cols = ORDER[part][VIA[slot]], pl.ds(*MIXED_COLS[part])
        return remote(xall.at[SOURCE[slot], :, cols], xall.at[slot + 1, :, cols], snd.at[0], gr.at[slot], dev(BIT[axis]))

    def mixed_start(*slots):
        for slot in slots:
            for part in AXES:
                mixed_copy(part, slot).start()

    def mixed_give(v):
        remote(xall.at[v], xall.at[8 + v], snd.at[0], dr.at[v], twin).start()

    def mixed_take(sems, n):
        remote(xall.at[0], xall.at[0], snd.at[0], sems.at[n], me).wait_recv()

    def mixed_product(i):
        v, other = mixed_order(i)
        return lax.dot_general(xall[8 * other + v], abuf[i % RING], NT, preferred_element_type=F32)

    def mixed_refill(i):
        @pl.when(i < NDEV - RING)
        def _():
            load_mixed(i + RING, i % RING)

        @pl.when(i >= NDEV - RING)
        def _():
            load_a(i + RING - NDEV, i % RING).start()

    def aggregate_features():
        wait_a(0)
        s1acc[0:FROWS, :] += mixed_product(0)
        mixed_refill(0)

        @pl.loop(0, 7)
        def _(slot):
            for k in range(7):
                @pl.when(slot == k)
                def _():
                    mixed_take(gr, k)
                    mixed_start(*(later for later in range(3, 7) if SOURCE[later] == k + 1))
                    mixed_give(k + 1)
            mixed_take(dr, slot)
            i = 2 * slot + 1
            wait_a(i % RING)
            wait_a((i + 1) % RING)
            s1acc[0:FROWS, :] += mixed_product(i) + mixed_product(i + 1)
            mixed_refill(i)
            mixed_refill(i + 1)

        mixed_take(dr, 7)
        wait_a((NDEV - 1) % RING)
        s1acc[0:FROWS, :] += mixed_product(NDEV - 1)
        mixed_refill(NDEV - 1)

    def gather(buf, g):
        def piece(owner, part):
            return buf.at[owner, pl.ds(*GATHER_ROWS[part])]

        def copy(axis, slot):
            part, mask = gather_unit(axis, slot)
            ref = piece(dev(mask), part)
            n = 7 + (slot if slot < 4 else 4 if slot == 6 else 2 * axis + slot + 1)
            return remote(ref, ref, snd.at[g], gr.at[n], dev(BIT[axis]))

        def whole(sems, n):
            return remote(buf.at[me], buf.at[me], snd.at[g], sems.at[n], me)

        def give(*masks):
            for mask in masks:
                owner = dev(mask)
                for ref in [buf.at[owner]] if mask < 7 else [piece(owner, part) for part in AXES]:
                    remote(ref, ref, snd.at[g], dr.at[8 + mask], twin).start()

        def take(*masks):
            for mask in masks:
                whole(dr, 8 + mask).wait_recv()

        def begin():
            for slot in AXES:
                for axis in AXES:
                    copy(axis, slot).start()
            give(0)

        def forward(axis, slot, *onto):
            part, mask = gather_unit(axis, slot)
            for over, later in onto:
                assert gather_unit(over, later) == (part, mask | BIT[axis])
                copy(over, later).start()

        def arrive(*slots):
            for slot in slots:
                whole(gr, 7 + min(slot, 4)).wait_recv()

        def arrive_one(axis, slot):
            part, mask = gather_unit(axis, slot)
            ref = piece(dev(mask | BIT[axis]), part)
            remote(ref, ref, snd.at[g], gr.at[8 + 2 * axis + slot], me).wait_recv()

        def hooks(p):
            @pl.when(p == 0)
            def _():
                take(0)

            @pl.when(p == 1)
            def _():
                for slot in AXES:
                    arrive(slot)
                    for over in AXES:
                        if slot == 0:
                            forward((over + 2) % 3, 0, (over, 3))
                        if slot == 1:
                            forward((over + 2) % 3, 1, (over, 5))
                        if (slot == 0) == (over != 1) and slot < 2:
                            forward((over + 1) % 3, 0, (over, 4))
                give(1, 2, 4)

            @pl.when(p == 2)
            def _():
                take(1)

            @pl.when(p == 3)
            def _():
                take(2, 4)

            @pl.when(p == 4)
            def _():
                arrive(3)
                for over in AXES:
                    forward((over + 2) % 3, 3, (over, 6))
                arrive_one(1, 5)
                arrive_one(0, 4)
                give(3)
                take(3)

            @pl.when(p == 5)
            def _():
                arrive_one(2, 4)
                arrive_one(1, 4)
                arrive_one(0, 5)
                arrive_one(2, 5)
                give(5, 6)

            @pl.when(p == 6)
            def _():
                take(5, 6)

        def tail(i):
            if i:
                take(7)
            else:
                arrive(6)
                give(7)

        return begin, hooks, tail

    def drain(buf, n):
        every = buf.at[pl.ds(0, 15)]
        remote(every, every, snd.at[n], gr.at[n], me).wait_send()

    def aggregate(buf, total, hooks, tail):
        def product(i):
            return jnp.dot(abuf[(NDEV + i) % RING], buf[block_of(i)], preferred_element_type=F32)

        def refill(i):
            @pl.when(i < NDEV - RING)
            def _():
                load_a(i + RING, (NDEV + i) % RING).start()

        @pl.loop(0, 7)
        def _(p):
            hooks(p)
            for k in BOTH:
                wait_a((NDEV + 2 * p + k) % RING)
            total[...] += product(2 * p) + product(2 * p + 1)
            for k in BOTH:
                refill(2 * p + k)

        for k in BOTH:
            tail(k)
            wait_a((NDEV + 14 + k) % RING)
            result = total[...] + product(14 + k)
            if k:
                return result
            total[...] = result

    def small(x, src, dst, scatter=False):
        for d in far_first:
            remote(src.at[peer(d)] if scatter else src, dst.at[me], snd.at[3 + x], pr.at[x], peer(d)).start()

    def small_wait(x, dst):
        ref = dst.at[pl.ds(0, 15)]
        remote(ref, ref, snd.at[3 + x], pr.at[x], me).wait()

    begin_h, hooks_h, tail_h = gather(hall, 1)

    mixed_start(0, 1, 2)
    mixed_give(0)
    for load in loads[2:]:
        load.wait()
    w1p[...] = jnp.zeros_like(w1p)
    w1p[0:FIN, :] = w1_ref[...]
    w1t[...] = w1p[...].T.astype(BF16)
    w2t[...] = jnp.zeros_like(w2t)
    w2t[0:NCLS, :] = w2_ref[...].astype(BF16)
    s1acc[...] = jnp.zeros_like(s1acc)
    s2acc[...] = jnp.zeros_like(s2acc)
    aggregate_features()

    s1b[...] = s1acc[...].astype(BF16)
    pre_one = jnp.dot(s1acc[...].T.astype(BF16), w1p[...].astype(BF16), preferred_element_type=F32)
    hall[me] = jnp.maximum(pre_one, 0.0).astype(BF16)
    begin_h()
    small(0, cnt.at[me], cnt)
    z1t[...] = jnp.dot(w1t[...], s1b[...], preferred_element_type=F32)
    s2b[...] = aggregate(hall, s2acc, hooks_h, tail_h).astype(BF16)

    small_wait(0, cnt)
    label_count = jnp.sum(cnt[...], axis=0)[0:1, 0:1]
    logits = lax.dot_general(w2t[...], s2b[...], NT, preferred_element_type=F32)
    classes = lax.broadcasted_iota(jnp.int32, (CPAD, BLK), 0)
    logits = jnp.where(classes < NCLS, logits, -jnp.inf)
    shifted = logits - jnp.max(logits, axis=0, keepdims=True)
    log_prob = shifted - jnp.log(jnp.sum(jnp.exp(shifted), axis=0, keepdims=True))
    hit = classes == y_ref[...]
    weight = m_ref[...].astype(F32)
    picked = jnp.sum(jnp.where(hit, log_prob, 0.0), axis=0, keepdims=True)
    loss_part = -jnp.sum(weight * picked)
    grad = weight * (jnp.exp(log_prob) - jnp.where(hit, 1.0, 0.0)) / label_count
    gt[...] = grad.astype(BF16)
    ut[...] = lax.dot_general(w2t[...], gt[...], TN, preferred_element_type=F32).astype(BF16)

    def pair_sum(mask, quarter=None):
        if quarter is None:
            return remote(acc.at[8 + mask], drecv.at[mask], snd.at[2], er.at[mask], twin)
        cols = pl.ds(quarter * 256, 256)
        return remote(acc.at[8 + mask, :, cols], drecv.at[mask, :, cols], snd.at[2], er.at[mask + quarter],
                      twin)

    def unit_copy(part, k, quarter=None):
        axis, mask = reduce_unit(part, k)
        rows = pl.ds(*REDUCE_ROWS[part])
        if quarter is None:
            return remote(acc.at[mask, rows], rbuf.at[k, rows], snd.at[2], rr.at[k], dev(BIT[axis]))
        cols = pl.ds(quarter * 256, 256)
        return remote(acc.at[mask, rows, cols], rbuf.at[k, rows, cols], snd.at[2], rr.at[k], dev(BIT[axis]))

    def add_rows(mask, source, start, size, cols=slice(None)):
        @pl.loop(0, size // 8)
        def _(t):
            rows = pl.ds(pl.multiple_of(start + t * 8, 8), 8)
            acc[mask, rows, cols] += source[rows, cols]

    def take_pair(mask):
        pair_sum(mask).wait_recv()
        add_rows(mask, drecv.at[mask], 0, HID)
        for k in range(1, 4):
            for part in AXES:
                if reduce_unit(part, k)[1] == mask:
                    unit_copy(part, k).start()

    for other in (1, 0):
        for q in QUARTERS:
            cols = pl.ds(q * 256, 256)
            acc[7 + 8 * other, :, cols] = jnp.dot(ut[...], abuf[(30 + other) % RING, :, cols],
                                                  preferred_element_type=F32)
            if other:
                pair_sum(7, q).start()

    for j in BOTH:
        load_a(NDEV - 1 - j - RING, (31 - j) % RING).start()

    for q in QUARTERS:
        pair_sum(7, q).wait_recv()
        cols = pl.ds(q * 256, 256)
        acc[7, :, cols] += drecv[7, :, cols]
        for part in AXES:
            unit_copy(part, 0, q).start()

    @pl.loop(1, 8)
    def _(p):
        for k in BOTH:
            @pl.when(p >= 3)
            def _():
                wait_a((31 - 2 * p - k) % RING)
        for k in BOTH:
            mask, other = step_order(NDEV - 1 - 2 * p - k)
            acc[mask + 8 * other] = jnp.dot(ut[...], abuf[(31 - 2 * p - k) % RING], preferred_element_type=F32)
        for k in BOTH:
            @pl.when(p < 5)
            def _():
                load_a(NDEV - 1 - 2 * p - k - RING, (31 - 2 * p - k) % RING).start()

        for step in range(2, NDEV):
            step_mask, step_other = step_order(NDEV - 1 - step)

            @pl.when(p == step // 2)
            def _():
                if step_other:
                    pair_sum(step_mask).start()
                else:
                    take_pair(step_mask)

    def units_wait(k):
        remote(rbuf.at[k], rbuf.at[k], snd.at[2], rr.at[k], me).wait_recv()

    def take_units(k, send=None):
        units_wait(k)
        for part in AXES:
            axis, mask = reduce_unit(part, k)
            add_rows(mask - BIT[axis], rbuf.at[k], *REDUCE_ROWS[part])
            if send is not None:
                unit_copy(part, send).start()

    take_units(0, 4)
    take_units(1, 5)
    take_units(2)
    take_units(3)
    take_units(4, 6)
    dw2_part = jnp.dot(gt[...], s2b[...], preferred_element_type=F32)
    d2src[...] = jnp.zeros_like(d2src)
    for j in range(6):
        for k in BOTH:
            d2src[6 * k + j] = dw2_part[j * 8:(j + 1) * 8, k * 128:(k + 1) * 128]
    d2src[12] = jnp.full(TILE, loss_part, F32)
    d2src[13] = jnp.full(TILE, jnp.sum(weight), F32)
    keep_two = pltpu.make_async_copy(d2r2, d2out.at[me], xsem.at[0])
    d2r1[me] = d2src[me]
    small(1, d2src, d2r1, True)
    take_units(5)
    units_wait(6)
    grad_one = jnp.where(z1t[...] > 0.0, acc[0] + rbuf[6], 0.0).astype(BF16)
    d1src[...] = lax.dot_general(grad_one, s1b[...], NT, preferred_element_type=F32).reshape(NDEV, 16, FPAD)
    d1r1[me] = d1src[me]
    small(3, d1src, d1r1, True)
    small_wait(1, d2r1)
    d2r2[...] = jnp.sum(d2r1[...], axis=0)
    small(2, d2r2, d2out)
    keep_two.start()
    for n, buf in enumerate((xall, hall, acc)):
        drain(buf, n)
    small_wait(3, d1r1)
    d1r2[...] = jnp.sum(d1r1[...], axis=0)
    small(4, d1r2, d1out)
    keep_one = pltpu.make_async_copy(d1r2, d1out.at[me], xsem.at[1])
    keep_one.start()
    small_wait(2, d2out)
    keep_two.wait()
    keep_one.wait()
    small_wait(4, d1out)


def finish(d1_ref, d2_ref, loss_out, dw1_out, dw2_out):
    loss_out[...] = d2_ref[12, 0:1, 0:1] / d2_ref[13, 0:1, 0:1]
    dw1_out[...] = d1_ref[...].reshape(HID, FPAD).T[0:FIN, :]
    for k in BOTH:
        dw2_out[:, pl.ds(k * 128, 128)] = d2_ref[pl.ds(6 * k, 6)].reshape(CPAD, 128)[0:NCLS]


def solution(mesh):
    def local_step(adj_rows, feat_rows, w_one, w_two, label_rows, mask_rows):
        vmem = pl.BlockSpec(memory_space=pltpu.VMEM)
        hbm = pl.BlockSpec(memory_space=pl.ANY)
        dma = pltpu.SemaphoreType.DMA
        parts = pl.pallas_call(
            kernel,
            out_shape=(jax.ShapeDtypeStruct((NDEV, 16, FPAD), F32), jax.ShapeDtypeStruct((NDEV, *TILE), F32)),
            in_specs=[hbm] * 6,
            out_specs=(hbm, hbm),
            scratch_shapes=[
                pltpu.VMEM((RING, BLK, BLK), BF16),
                pltpu.VMEM((FIN, BLK), BF16),
                pltpu.VMEM((FIN, HID), F32),
                pltpu.VMEM((NCLS, HID), F32),
                pltpu.VMEM((1, BLK), jnp.int32),
                pltpu.VMEM((1, BLK), jnp.int32),
                pltpu.VMEM((NDEV, FROWS, BLK), BF16),
                pltpu.VMEM((NDEV, BLK, HID), BF16),
                pltpu.VMEM((FPAD, BLK), F32),
                pltpu.VMEM((BLK, HID), F32),
                pltpu.VMEM((FPAD, BLK), BF16),
                pltpu.VMEM((BLK, HID), BF16),
                pltpu.VMEM((HID, BLK), F32),
                pltpu.VMEM((FPAD, HID), F32),
                pltpu.VMEM((HID, FPAD), BF16),
                pltpu.VMEM((CPAD, HID), BF16),
                pltpu.VMEM((HID, BLK), BF16),
                pltpu.VMEM((16, HID, BLK), F32),
                pltpu.VMEM((8, HID, BLK), F32),
                pltpu.VMEM((7, HID, BLK), F32),
                pltpu.VMEM((CPAD, BLK), BF16),
                pltpu.VMEM((NDEV, 1, 128), F32),
                *[pltpu.VMEM((NDEV, *TILE), F32)] * 2,
                pltpu.VMEM(TILE, F32),
                *[pltpu.VMEM((NDEV, 16, FPAD), F32)] * 2,
                pltpu.VMEM((16, FPAD), F32),
                *[dma((n,)) for n in (RING, 5, 18, 16, 7, 11, 5, 8)],
            ],
            compiler_params=pltpu.CompilerParams(collective_id=0, has_side_effects=True,
                                                 vmem_limit_bytes=67 * 1000 * 1000),
        )(adj_rows, feat_rows.T, w_one, w_two.T, label_rows.reshape(1, BLK), mask_rows.reshape(1, BLK))
        loss, dw_one, dw_two = pl.pallas_call(
            finish,
            out_shape=(jax.ShapeDtypeStruct((1, 1), F32), jax.ShapeDtypeStruct((FIN, HID), F32),
                       jax.ShapeDtypeStruct((NCLS, HID), F32)),
            in_specs=[vmem] * 2,
            out_specs=(vmem, vmem, vmem),
        )(*parts)
        return loss.reshape(1), dw_one, dw_two.T

    return jax.shard_map(local_step, mesh=mesh,
                         in_specs=(P(AXIS, None), P(AXIS, None), P(None, None), P(None, None), P(AXIS), P(AXIS)),
                         out_specs=(P(None), P(None, None), P(None, None)), check_vma=False)
```
